256 devices in a mesh: pulse: 8 (over y_lo, x), tile: 32 (over z, y_hi, core).
Axes of the slice: x: 4, y: 4 (y_hi: 2, y_lo: 2; y = y_hi * 2 + y_lo), z: 8, core: 2. Of those that a mesh axis runs over, the one named last changes fastest.
Arguments:
- pulses: bfloat16 [4096, 2, 32768], P(None, None, ('pulse', 'tile')), may hold values from -6 to 6
- steering: bfloat16 [2, 128, 128], replicated, may hold values from -0.375 to 0.375
- merge_re: bfloat16 [3, 256, 256], replicated, may hold values from -0.25 to 0.25
- merge_im: bfloat16 [3, 256, 256], replicated, may hold values from -0.25 to 0.25
- range_shift: int32 [3, 2, 128], replicated, may hold values from -8 to 8
- image_map: bfloat16 [8, 32, 2, 128, 512], P('pulse', 'tile'), may hold values from -0.0234375 to 0.0234375
Outputs:
- image: float32 [4096, 1024], P(('pulse', 'tile'))
The draws below stay inside these ranges and needn't reach their ends.
All inputs are finite; a program needn't handle non-finite values.
Results may differ from the reference program's by a relative error of at most 0.0057.
Values may be sent and summed in bfloat16 or wider, within the bound.
No kernel may reach another device: no remote copies, remote signals or barrier semaphores. Data moves between devices by JAX's collectives and lax.ppermute only.
A program may use at most 64 MiB of HBM per device.

```python
import jax
import jax.numpy as jnp
import numpy as np
from jax import lax

R = 4096
PD = 128
K = 128
X = 512
LEVELS = 3
SHIFT = 8
GROUPS = 8
SUBS = 32
N_PULSE = 8
N_TILE = 32
DEVICES = 256


def place_ends(array, own_key, low, largest):
    place = [jax.random.randint(jax.random.fold_in(own_key, axis), (), 0, length) for axis, length in enumerate(array.shape)]
    main_axis = array.shape.index(max(array.shape))
    neighbour = place[:main_axis] + [(place[main_axis] + 1) % array.shape[main_axis]] + place[main_axis + 1:]
    return array.at[tuple(place)].set(low).at[tuple(neighbour)].set(largest)


def levels(rng, shape, split, least, high):
    loudness, own = 1.0, jax.random.fold_in(rng, 6)
    for axis_at, blocks in split:
        steps = jnp.exp(jax.random.uniform(jax.random.fold_in(own, axis_at), (blocks,), jnp.float32, least / len(split), high / len(split)))
        loudness = loudness * jnp.repeat(steps, shape[axis_at] // blocks).reshape([-1 if axis == axis_at else 1 for axis in range(len(shape))])
    return loudness


def scatter_about(stream_key, shape, spread, limit, cuts=(), kind=jnp.bfloat16):
    entries = jax.random.normal(stream_key, shape, jnp.float32) * spread
    if len(cuts) > 0:
        entries = levels(stream_key, shape, cuts, -0.22, 0.18) * entries
    return jnp.clip(entries, min=-limit, max=limit).astype(kind)


def setup_inputs(seed: int = 0) -> dict:
    key_list = jax.random.split(jax.random.key(seed), 7)
    pulses = scatter_about(key_list[0], (R, 2, PD * DEVICES), 1.0, 6.0, ((2, 256),))
    steering = scatter_about(key_list[1], (2, PD, K), (2 * PD) ** -0.5, 0.375)
    merge_re = scatter_about(key_list[2], (LEVELS, 2 * K, 2 * K), (4 * K) ** -0.5, 0.25)
    merge_im = scatter_about(key_list[3], (LEVELS, 2 * K, 2 * K), (4 * K) ** -0.5, 0.25)
    range_shift = place_ends(jax.random.randint(key_list[4], (LEVELS, 2, K), 0 - SHIFT, SHIFT + 1), jax.random.fold_in(key_list[4], 1), 0 - SHIFT, SHIFT).astype(jnp.int32)
    image_map = scatter_about(key_list[5], (GROUPS, SUBS, 2, K, X), (2 * K * DEVICES) ** -0.5, 0.0234375, ((0, 8), (1, 32)))
    return {"pulses": pulses, "steering": steering, "merge_re": merge_re, "merge_im": merge_im, "range_shift": range_shift, "image_map": image_map}


def complex_block(real_part, imag_part):
    upper_half = jnp.concatenate([real_part, imag_part], axis=1)
    lower_half = jnp.concatenate([-imag_part, real_part], axis=1)
    return jnp.concatenate([upper_half, lower_half], axis=0)


def shift_rows(beam_rows, shift_table):
    range_rows = beam_rows.shape[0]
    doubled = jnp.concatenate([shift_table, shift_table]).astype(jnp.int32)
    source = jnp.arange(range_rows, dtype=jnp.int32)[:, None] + doubled[None, :]
    inside = (source >= 0) & (source < range_rows)
    picked = jnp.take_along_axis(beam_rows, jnp.clip(source, 0, range_rows - 1), axis=0)
    return jnp.where(inside, picked, jnp.zeros_like(picked))


def reference(pulses, steering, merge_re, merge_im, range_shift, image_map):
    steer_block = complex_block(steering[0], steering[1]).astype(jnp.float32)
    shaped = pulses.reshape(R, 2, N_PULSE, N_TILE, PD).transpose(2, 3, 0, 1, 4).reshape(N_PULSE, N_TILE, R, 2 * PD)
    level_blocks = []
    for merge_level in range(LEVELS):
        chosen = []
        for half_bit in range(2):
            weight_re = merge_re[merge_level][:, half_bit * K:(half_bit + 1) * K]
            weight_im = merge_im[merge_level][:, half_bit * K:(half_bit + 1) * K]
            chosen.append(complex_block(weight_re, weight_im))
        level_blocks.append(jnp.stack(chosen))

    def group_term(running_sum, inputs):
        pulse_block, group_maps = inputs
        current = jnp.einsum("srp,pk->srk", pulse_block.astype(jnp.float32), steer_block).astype(jnp.bfloat16)
        for merge_level in range(LEVELS):
            partner_index = np.arange(N_TILE) ^ (1 << merge_level)
            halves = (np.arange(N_TILE) >> merge_level) & 1
            partner = current[partner_index]
            is_upper = jnp.asarray(halves == 1)[:, None, None]
            lower_src = jnp.where(is_upper, partner, current)
            upper_src = jnp.where(is_upper, current, partner)
            shifted_lower = jax.vmap(shift_rows, (0, None))(lower_src, range_shift[merge_level, 0])
            shifted_upper = jax.vmap(shift_rows, (0, None))(upper_src, range_shift[merge_level, 1])
            combined = jnp.concatenate([shifted_lower[..., :K], shifted_upper[..., :K], shifted_lower[..., K:], shifted_upper[..., K:]], axis=-1)
            per_sub = level_blocks[merge_level][halves]
            current = jnp.einsum("srk,skn->srn", combined.astype(jnp.float32), per_sub.astype(jnp.float32)).astype(jnp.bfloat16)
        map_blocks = jax.vmap(complex_block)(group_maps[:, 0], group_maps[:, 1])
        contribution = jnp.einsum("srk,skx->rx", current.astype(jnp.float32), map_blocks.astype(jnp.float32))
        return running_sum + contribution, None

    start_sum = jnp.zeros((R, 2 * X), jnp.float32)
    image, _ = lax.scan(group_term, start_sum, (shaped, image_map))
    return image
```

```python
import functools

import jax
import jax.numpy as jnp
from jax import lax
from jax.experimental import pallas as pl
from jax.experimental.pallas import tpu as pltpu
from jax.sharding import PartitionSpec as P

SHIFT = 8
SET = 8


def complex_block(real_part, imag_part):
    upper_half = jnp.concatenate([real_part, imag_part], axis=1)
    lower_half = jnp.concatenate([-imag_part, real_part], axis=1)
    return jnp.concatenate([upper_half, lower_half], axis=0)


def form_kernel(
    rows, own, member_ref, windows_ref, steer_ref, merge_ref, shift_ref, *rest
):
    maps, (out_ref, beams, sources, stacked) = rest[:SET], rest[SET:]
    levels = merge_ref.shape[0]
    count = steer_ref.shape[1] // 2
    member = member_ref[0]
    chunk = 80
    guard = jnp.zeros((SHIFT, count), jnp.float32)

    def first(index, carry):
        for part in range(2):
            beams[index, part, pl.ds(0, SHIFT), :] = guard
            beams[index, part, pl.ds(SHIFT + rows, SHIFT), :] = guard
        result = jnp.dot(windows_ref[index], steer_ref[...], preferred_element_type=jnp.float32)
        result = result.astype(jnp.bfloat16).astype(jnp.float32)
        beams[index, 0, pl.ds(SHIFT, rows), :] = result[:, :count]
        beams[index, 1, pl.ds(SHIFT, rows), :] = result[:, count:]
        return carry

    lax.fori_loop(0, SET, first, 0)

    sublane = lax.broadcasted_iota(jnp.int32, (SHIFT, count), 0)
    for level in range(levels):
        picks, places = [], []
        for side in range(2):
            offset = jnp.broadcast_to(shift_ref[level, side : side + 1, :], (SHIFT, count)) + sublane
            picks.append(offset & (SHIFT - 1))
            places.append(offset >> 3)

        def pair(index, carry, level=level, picks=picks, places=places):
            low = ((index >> level) << (level + 1)) | (index & (2**level - 1))
            ends = (low, low | 2**level)

            def shift(step, carry):
                base = step * chunk
                for side in range(2):
                    before, after = places[side] < 0, places[side] > 0
                    for part in range(2):
                        turned = []
                        for tile in range(chunk // SHIFT + 2):
                            at = pl.multiple_of(base + tile * SHIFT, SHIFT)
                            value = beams[ends[side], part, pl.ds(at, SHIFT), :]
                            turned.append(jnp.take_along_axis(value, picks[side], axis=0))
                        moved = [
                            jnp.where(
                                before,
                                turned[tile],
                                jnp.where(after, turned[tile + 2], turned[tile + 1]),
                            )
                            for tile in range(chunk // SHIFT)
                        ]
                        column = (2 * part + side) * count
                        sources[pl.ds(pl.multiple_of(base, 16), chunk), column : column + count] = (
                            jnp.concatenate(moved, axis=0).astype(jnp.bfloat16)
                        )
                return carry

            lax.fori_loop(0, rows // chunk, shift, 0)
            for part in range(2):
                result = jnp.dot(
                    sources[...],
                    merge_ref[level, :, 2 * part * count : 2 * (part + 1) * count],
                    preferred_element_type=jnp.float32,
                )
                result = result.astype(jnp.bfloat16).astype(jnp.float32)
                beams[ends[0], part, pl.ds(SHIFT, rows), :] = result[:, :count]
                beams[ends[1], part, pl.ds(SHIFT, rows), :] = result[:, count:]
            return carry

        lax.fori_loop(0, SET // 2, pair, 0)

    start = pl.multiple_of(jnp.clip(member * own - (rows - own) // 2, 0, SET * own - rows), SHIFT)
    at = pl.multiple_of(member * own - start + SHIFT, SHIFT)
    for slot in range(SET):
        real = beams[member ^ slot, 0, pl.ds(at, own), :].astype(jnp.bfloat16)
        imag = beams[member ^ slot, 1, pl.ds(at, own), :].astype(jnp.bfloat16)
        column = 2 * slot * count
        stacked[:own, column : column + count] = real
        stacked[:own, column + count : column + 2 * count] = -imag
        stacked[own:, column : column + count] = imag
        stacked[own:, column + count : column + 2 * count] = real
    width = maps[0].shape[1]
    for half in range(2):
        total = jnp.zeros((own, width), jnp.float32)
        for slot in range(SET):
            total += jnp.dot(
                stacked[half * own : (half + 1) * own, 2 * slot * count : 2 * (slot + 1) * count],
                maps[slot][...],
                preferred_element_type=jnp.float32,
            )
        out_ref[:, half * width : (half + 1) * width] = total.astype(jnp.bfloat16)


def body(pulses, steering, merge_re, merge_im, range_shift, image_map):
    total_rows = pulses.shape[0]
    count = steering.shape[2]
    levels = merge_re.shape[0]
    groups = lax.axis_size("pulse")
    tiles = lax.axis_size("tile")
    sets = tiles // SET
    own = total_rows // SET
    halo = levels * SHIFT
    rows = own + 2 * halo
    member = lax.axis_index("tile") % SET

    def swap(value, mask):
        return lax.ppermute(value, "tile", [(s, s ^ mask) for s in range(tiles)])

    pulse_rows = pulses.reshape(total_rows, -1)
    starts = [min(max(block * own - halo, 0), total_rows - rows) for block in range(SET)]
    windows = jnp.stack([pulse_rows[start : start + rows] for start in starts])
    members = [[base + k for k in range(SET)] for base in range(0, tiles, SET)]
    windows = lax.all_to_all(windows, "tile", 0, 0, axis_index_groups=members, tiled=True)

    own_map = image_map.reshape(2 * count, -1)
    held = {0: own_map}
    for mask in (4, 2, 1):
        for slot in list(held):
            held[slot | mask] = swap(held[slot], mask)

    steer_block = complex_block(steering[0], steering[1])
    merge_block = jnp.stack([complex_block(merge_re[l], merge_im[l]) for l in range(levels)])

    partial_rows = pl.pallas_call(
        functools.partial(form_kernel, rows, own),
        out_shape=jax.ShapeDtypeStruct((own, 2 * own_map.shape[1]), jnp.bfloat16),
        in_specs=[pl.BlockSpec(memory_space=pltpu.SMEM)]
        + [pl.BlockSpec(memory_space=pltpu.VMEM)] * (4 + SET),
        out_specs=pl.BlockSpec(memory_space=pltpu.VMEM),
        scratch_shapes=[
            pltpu.VMEM((SET, 2, rows + 2 * SHIFT, count), jnp.float32),
            pltpu.VMEM((rows, 4 * count), jnp.bfloat16),
            pltpu.VMEM((2 * own, 2 * SET * count), jnp.bfloat16),
        ],
        cost_estimate=pl.CostEstimate(flops=6 * 10**9, bytes_accessed=8 * 10**6, transcendentals=0),
        compiler_params=pltpu.CompilerParams(vmem_limit_bytes=48 * 2**20),
    )(
        member.reshape(1).astype(jnp.int32),
        windows,
        steer_block,
        merge_block,
        range_shift,
        *[held[slot] for slot in range(SET)],
    )

    pieces = lax.all_to_all(
        partial_rows.reshape(groups, own // groups, -1), "pulse", 0, 0, tiled=True
    )
    summed = jnp.sum(pieces.astype(jnp.float32), axis=0).astype(jnp.bfloat16)
    quarters = summed.reshape(sets, own // groups // sets, -1)
    which = lax.axis_index("tile") // SET
    result = None
    for turn in range(sets):
        pairs = []
        for g in range(groups):
            for t in range(tiles):
                u, i = t // SET, t % SET
                pairs.append((g * tiles + t, i * tiles + sets * g + (u + turn) % sets))
        block = lax.dynamic_index_in_dim(quarters, (which + turn) % sets, 0, keepdims=False)
        arrived = lax.ppermute(block, ("pulse", "tile"), pairs).astype(jnp.float32)
        result = arrived if result is None else result + arrived
    return result


def solution(mesh):
    placed = (
        P(None, None, ("pulse", "tile")),
        P(),
        P(),
        P(),
        P(),
        P("pulse", "tile", None, None, None),
    )
    return jax.shard_map(
        body, mesh=mesh, in_specs=placed, out_specs=P(("pulse", "tile"), None), check_vma=False
    )
```

```python
import functools

import jax
import jax.numpy as jnp
from jax import lax
from jax.experimental import pallas as pl
from jax.experimental.pallas import tpu as pltpu
from jax.sharding import PartitionSpec as P

SHIFT = 8
SET = 8
VMEM = pl.BlockSpec(memory_space=pltpu.VMEM)


def complex_block(real_part, imag_part):
    upper_half = jnp.concatenate([real_part, imag_part], axis=1)
    lower_half = jnp.concatenate([-imag_part, real_part], axis=1)
    return jnp.concatenate([upper_half, lower_half], axis=0)


def merge_kernel(
    own, halo, member_ref, block_ref, edge_ref, steer_ref, merge_ref, shift_ref, out_ref,
    beams, sources, spread
):
    levels = merge_ref.shape[0]
    count = steer_ref.shape[1] // 2
    rows = own + 2 * halo
    member = member_ref[0]
    chunk = 80

    def clear(index, low, length):
        for part in range(2):
            beams[index, part, pl.ds(low, length), :] = jnp.zeros((length, count), jnp.float32)

    def clear_outside(index):
        @pl.when(member == 0)
        def _():
            clear(index, SHIFT, halo)

        @pl.when(member == SET - 1)
        def _():
            clear(index, SHIFT + halo + own, halo)

    def first(index, carry):
        clear(index, 0, SHIFT)
        clear(index, SHIFT + rows, SHIFT)
        spread[: 2 * halo, :] = edge_ref[index, : 2 * halo, :].astype(jnp.float32)
        spread[2 * halo : 2 * (halo + own), :] = block_ref[index].astype(jnp.float32)
        spread[2 * (halo + own) :, :] = edge_ref[index, 2 * halo :, :].astype(jnp.float32)
        real = spread[pl.ds(0, rows, stride=2), :].astype(jnp.bfloat16)
        imag = spread[pl.ds(1, rows, stride=2), :].astype(jnp.bfloat16)
        result = jnp.dot(
            jnp.concatenate([real, imag], axis=1), steer_ref[...], preferred_element_type=jnp.float32
        )
        beams[index, 0, pl.ds(SHIFT, rows), :] = result[:, :count]
        beams[index, 1, pl.ds(SHIFT, rows), :] = result[:, count:]
        return carry

    lax.fori_loop(0, SET, first, 0)

    sublane = lax.broadcasted_iota(jnp.int32, (SHIFT, count), 0)
    for level in range(levels):
        picks, places = [], []
        for side in range(2):
            offset = jnp.broadcast_to(shift_ref[level, side : side + 1, :], (SHIFT, count)) + sublane
            picks.append(offset & (SHIFT - 1))
            places.append(offset >> 3)

        def pair(index, carry, level=level, picks=picks, places=places):
            low = ((index >> level) << (level + 1)) | (index & (2**level - 1))
            ends = (low, low | 2**level)

            def shift(step, carry):
                base = step * chunk
                for side in range(2):
                    before, after = places[side] < 0, places[side] > 0
                    for part in range(2):
                        turned = []
                        for tile in range(chunk // SHIFT + 2):
                            at = pl.multiple_of(base + tile * SHIFT, SHIFT)
                            value = beams[ends[side], part, pl.ds(at, SHIFT), :]
                            turned.append(jnp.take_along_axis(value, picks[side], axis=0))
                        moved = [
                            jnp.where(
                                before,
                                turned[tile],
                                jnp.where(after, turned[tile + 2], turned[tile + 1]),
                            )
                            for tile in range(chunk // SHIFT)
                        ]
                        column = (2 * part + side) * count
                        sources[pl.ds(pl.multiple_of(base, 16), chunk), column : column + count] = (
                            jnp.concatenate(moved, axis=0).astype(jnp.bfloat16)
                        )
                return carry

            lax.fori_loop(0, rows // chunk, shift, 0)
            for part in range(2):
                result = jnp.dot(
                    sources[...],
                    merge_ref[level, :, 2 * part * count : 2 * (part + 1) * count],
                    preferred_element_type=jnp.float32,
                )
                if level < levels - 1:
                    beams[ends[0], part, pl.ds(SHIFT, rows), :] = result[:, :count]
                    beams[ends[1], part, pl.ds(SHIFT, rows), :] = result[:, count:]
                else:
                    for side in range(2):
                        kept = result[halo : halo + own, side * count : (side + 1) * count]
                        out_ref[ends[side] ^ member, part] = kept.astype(jnp.bfloat16)
            if level < levels - 1:
                clear_outside(ends[0])
                clear_outside(ends[1])
            return carry

        lax.fori_loop(0, SET // 2, pair, 0)


def image_kernel(groups, beams_ref, *rest):
    maps, out_ref = rest[:SET], rest[SET]
    own, count = beams_ref.shape[2], beams_ref.shape[3]
    width = maps[0].shape[1]
    piece = out_ref.shape[2]
    for half in range(2):
        total = jnp.zeros((own, width), jnp.float32)
        for slot in range(SET):
            real, imag = beams_ref[slot, 0], beams_ref[slot, 1]
            left = jnp.concatenate([real, -imag] if half == 0 else [imag, real], axis=1)
            total += jnp.dot(left, maps[slot][...], preferred_element_type=jnp.float32)
        total = total.astype(jnp.bfloat16)
        for at in range(own // piece):
            out_ref[at % groups, at // groups, :, half * width : (half + 1) * width] = total[
                at * piece : (at + 1) * piece
            ]


def sum_kernel(pieces_ref, out_ref):
    total = pieces_ref[0].astype(jnp.float32)
    for source in range(1, pieces_ref.shape[0]):
        total += pieces_ref[source].astype(jnp.float32)
    total = total.astype(jnp.bfloat16)
    out_ref[0] = total
    out_ref[1] = total


def last_kernel(half_ref, pieces_ref, out_ref):
    many = pieces_ref.shape[0] // 2
    base = half_ref[0] * many
    total = pieces_ref[base].astype(jnp.float32)
    for source in range(1, many):
        total += pieces_ref[base + source].astype(jnp.float32)
    out_ref[...] = total


def body(pulses, steering, merge_re, merge_im, range_shift, image_map):
    total_rows = pulses.shape[0]
    count = steering.shape[2]
    levels = merge_re.shape[0]
    groups = lax.axis_size("pulse")
    tiles = lax.axis_size("tile")
    sets = tiles // SET
    own = total_rows // SET
    halo = levels * SHIFT
    piece = own // tiles
    member = lax.axis_index("tile") % SET

    def swap(value, mask):
        return lax.ppermute(value, "tile", [(s, s ^ mask) for s in range(tiles)])

    raw = pulses.reshape(SET, 2 * own, -1)
    members = [[base + k for k in range(SET)] for base in range(0, tiles, SET)]
    blocks = lax.all_to_all(raw, "tile", 0, 0, axis_index_groups=members, tiled=True)
    none = jnp.zeros((1, 2 * halo, raw.shape[2]), raw.dtype)
    edges = jnp.concatenate(
        [
            jnp.concatenate([none, raw[:-1, -2 * halo :]], axis=0),
            jnp.concatenate([raw[1:, : 2 * halo], none], axis=0),
        ],
        axis=1,
    )
    edges = lax.all_to_all(edges, "tile", 0, 0, axis_index_groups=members, tiled=True)

    own_map = image_map.reshape(2 * count, -1)
    held = {0: own_map}
    for mask in (4, 2, 1):
        for slot in list(held):
            held[slot | mask] = swap(held[slot], mask)

    steer_block = complex_block(steering[0], steering[1])
    merge_block = jnp.stack([complex_block(merge_re[l], merge_im[l]) for l in range(levels)])

    rows = own + 2 * halo
    beams = pl.pallas_call(
        functools.partial(merge_kernel, own, halo),
        out_shape=jax.ShapeDtypeStruct((SET, 2, own, count), jnp.bfloat16),
        in_specs=[pl.BlockSpec(memory_space=pltpu.SMEM)] + [VMEM] * 5,
        out_specs=VMEM,
        scratch_shapes=[
            pltpu.VMEM((SET, 2, rows + 2 * SHIFT, count), jnp.float32),
            pltpu.VMEM((rows, 4 * count), jnp.bfloat16),
            pltpu.VMEM((2 * rows, count), jnp.float32),
        ],
        cost_estimate=pl.CostEstimate(flops=4 * 10**9, bytes_accessed=4 * 10**6, transcendentals=0),
        compiler_params=pltpu.CompilerParams(vmem_limit_bytes=24 * 2**20),
        name="merge",
    )(member.reshape(1).astype(jnp.int32), blocks, edges, steer_block, merge_block, range_shift)

    width = own_map.shape[1]
    partial_rows = pl.pallas_call(
        functools.partial(image_kernel, groups),
        out_shape=jax.ShapeDtypeStruct((groups, sets, piece, 2 * width), jnp.bfloat16),
        in_specs=[VMEM] * (1 + SET),
        out_specs=VMEM,
        cost_estimate=pl.CostEstimate(flops=2 * 10**9, bytes_accessed=4 * 10**6, transcendentals=0),
        compiler_params=pltpu.CompilerParams(vmem_limit_bytes=24 * 2**20),
        name="image",
    )(beams, *[held[slot] for slot in range(SET)])

    pieces = lax.all_to_all(partial_rows, "pulse", 0, 0, tiled=True)
    doubled = pl.pallas_call(
        sum_kernel,
        out_shape=jax.ShapeDtypeStruct((2, sets, piece, 2 * width), jnp.bfloat16),
        in_specs=[VMEM],
        out_specs=VMEM,
        name="sum",
    )(pieces)

    def device(pulse, u, i):
        return pulse * tiles + u * SET + i

    crossing = []
    for a in range(groups):
        for b in range(a + 1, groups):
            crossing.append(
                [device(a, u, b) for u in range(sets)] + [device(b, u, a) for u in range(sets)]
            )
    for a in range(0, groups, 2):
        crossing.append(
            [device(a, u, a) for u in range(sets)] + [device(a + 1, u, a + 1) for u in range(sets)]
        )
    last = lax.all_to_all(
        doubled.reshape(2 * sets, piece, 2 * width),
        ("pulse", "tile"),
        0,
        0,
        axis_index_groups=crossing,
        tiled=True,
    )
    pulse = lax.axis_index("pulse")
    half = jnp.where(pulse == member, pulse % 2, (pulse < member).astype(jnp.int32))
    return pl.pallas_call(
        last_kernel,
        out_shape=jax.ShapeDtypeStruct((piece, 2 * width), jnp.float32),
        in_specs=[pl.BlockSpec(memory_space=pltpu.SMEM), VMEM],
        out_specs=VMEM,
        name="last",
    )(half.reshape(1).astype(jnp.int32), last)


def solution(mesh):
    placed = (
        P(None, None, ("pulse", "tile")),
        P(),
        P(),
        P(),
        P(),
        P("pulse", "tile", None, None, None),
    )
    return jax.shard_map(
        body, mesh=mesh, in_specs=placed, out_specs=P(("pulse", "tile"), None), check_vma=False
    )
```

```python
import functools

import jax
import jax.numpy as jnp
from jax import lax
from jax.experimental import pallas as pl
from jax.experimental.pallas import tpu as pltpu
from jax.sharding import PartitionSpec as P

SHIFT = 8
SET = 8
VMEM = pl.BlockSpec(memory_space=pltpu.VMEM)
SMEM = pl.BlockSpec(memory_space=pltpu.SMEM)


def weights_kernel(steering_ref, merge_re_ref, merge_im_ref, steer_ref, merge_ref):
    def block(out, real, imag):
        high, wide = real.shape
        out[:high, :wide] = real
        out[:high, wide:] = imag
        out[high:, :wide] = -imag
        out[high:, wide:] = real

    block(steer_ref, steering_ref[0], steering_ref[1])
    for level in range(merge_re_ref.shape[0]):
        block(merge_ref.at[level], merge_re_ref[level], merge_im_ref[level])


def windows_kernel(own, halo, member_ref, raw_ref, *rest):
    outs, sems = rest[:SET], rest[SET]
    member = member_ref[0]
    main, edge = 2 * own, 2 * halo

    def copy(slot, kind, source, target, length):
        return pltpu.make_async_copy(
            raw_ref.at[pl.ds(pl.multiple_of(source, 16), length), :],
            outs[slot].at[pl.ds(target, length), :],
            sems.at[slot, kind],
        )

    def each(action):
        for slot in range(SET):
            block = member ^ slot
            start = block * main
            action(copy(slot, 0, start, edge, main))

            @pl.when(block > 0)
            def _():
                action(copy(slot, 1, start - edge, 0, edge))

            @pl.when(block < SET - 1)
            def _():
                action(copy(slot, 2, start + main, edge + main, edge))

    each(lambda made: made.start())
    zeros = jnp.zeros((edge, raw_ref.shape[1]), raw_ref.dtype)
    for slot in range(SET):
        block = member ^ slot

        @pl.when(block == 0)
        def _():
            outs[slot][:edge, :] = zeros

        @pl.when(block == SET - 1)
        def _():
            outs[slot][edge + main :, :] = zeros

    each(lambda made: made.wait())


def moved_rows(beams, slot, part, pick, before, after, base, chunk):
    value = beams[slot, part, pl.ds(base, chunk + 2 * SHIFT), :].astype(jnp.float32)
    turned = [
        jnp.take_along_axis(value[tile * SHIFT : (tile + 1) * SHIFT], pick, axis=0)
        for tile in range(chunk // SHIFT + 2)
    ]
    moved = [
        jnp.where(before, turned[tile], jnp.where(after, turned[tile + 2], turned[tile + 1]))
        for tile in range(chunk // SHIFT)
    ]
    return jnp.concatenate(moved, axis=0).astype(jnp.bfloat16)


def merge_level(own, halo, level, base_slots, member, beams, sources, merge, shift_ref, emit):
    count = beams.shape[-1]
    rows = own + 2 * halo
    chunk = 80
    sublane = lax.broadcasted_iota(jnp.int32, (SHIFT, count), 0)
    picks, befores, afters = [], [], []
    for side in range(2):
        offset = jnp.broadcast_to(shift_ref[level, side : side + 1, :], (SHIFT, count)) + sublane
        picks.append(offset & (SHIFT - 1))
        befores.append(offset < 0)
        afters.append(offset >= SHIFT)
    bit = (member >> level) & 1

    def pair(base):
        ends = (base + (bit << level), base + ((1 - bit) << level))

        def shift(step, carry):
            at = pl.multiple_of(step * chunk, 16)
            for side in range(2):
                for part in range(2):
                    column = (2 * part + side) * count
                    sources[pl.ds(at, chunk), column : column + count] = moved_rows(
                        beams, ends[side], part, picks[side], befores[side], afters[side], at, chunk
                    )
            return carry

        lax.fori_loop(0, rows // chunk, shift, 0)
        for part in range(2):
            result = jnp.dot(
                sources[...],
                merge[:, 2 * part * count : 2 * (part + 1) * count],
                preferred_element_type=jnp.float32,
            ).astype(jnp.bfloat16)
            for side in range(2):
                emit(ends[side], part, result[:, side * count : (side + 1) * count])

    if len(base_slots) == 1:
        pair(base_slots[0])
    else:
        def step(index, carry):
            low = ((index >> level) << (level + 1)) | (index & (2**level - 1))
            pair(low)
            return carry

        lax.fori_loop(0, len(base_slots), step, 0)


def start_kernel(own, halo, member_ref, left_ref, right_ref, steer_ref, merge_ref, shift_ref, out_ref,
                 beams, sources, spread):
    count = steer_ref.shape[1] // 2
    rows = own + 2 * halo
    member = member_ref[0]
    zeros = jnp.zeros((SHIFT, count), jnp.bfloat16)
    for slot, raw_ref in enumerate((left_ref, right_ref)):
        for part in range(2):
            beams[slot, part, :SHIFT, :] = zeros
            beams[slot, part, SHIFT + rows :, :] = zeros
            out_ref[slot, part, :SHIFT, :] = zeros
            out_ref[slot, part, SHIFT + rows :, :] = zeros
        spread[...] = raw_ref[...].astype(jnp.float32)
        real = spread[pl.ds(0, rows, stride=2), :].astype(jnp.bfloat16)
        imag = spread[pl.ds(1, rows, stride=2), :].astype(jnp.bfloat16)
        result = jnp.dot(
            jnp.concatenate([real, imag], axis=1), steer_ref[...], preferred_element_type=jnp.float32
        ).astype(jnp.bfloat16)
        beams[slot, 0, pl.ds(SHIFT, rows), :] = result[:, :count]
        beams[slot, 1, pl.ds(SHIFT, rows), :] = result[:, count:]

    def emit(slot, part, value):
        out_ref[slot, part, pl.ds(SHIFT, rows), :] = value

    merge_level(own, halo, 0, [0], member, beams, sources, merge_ref.at[0], shift_ref, emit)
    clear_outside(own, halo, member, out_ref, 2)


def clear_outside(own, halo, member, beams, slots):
    zeros = jnp.zeros((halo, beams.shape[-1]), beams.dtype)

    @pl.when(member == 0)
    def _():
        for slot in range(slots):
            for part in range(2):
                beams[slot, part, SHIFT : SHIFT + halo, :] = zeros

    @pl.when(member == SET - 1)
    def _():
        for slot in range(slots):
            for part in range(2):
                beams[slot, part, SHIFT + halo + own : SHIFT + 2 * halo + own, :] = zeros


def finish_kernel(own, halo, member_ref, *rest):
    pairs = rest[: SET // 2]
    merge_ref, shift_ref, out_ref, beams, sources = rest[SET // 2 :]
    rows = own + 2 * halo
    member = member_ref[0]
    for index in range(SET // 2):
        beams[2 * index : 2 * index + 2] = pairs[index][...]

    def keep(slot, part, value):
        beams[slot, part, pl.ds(SHIFT, rows), :] = value

    def last(slot, part, value):
        out_ref[slot, part] = value[halo : halo + own]

    bases = [0, 1, 4, 5]
    merge_level(own, halo, 1, bases, member, beams, sources, merge_ref.at[1], shift_ref, keep)
    clear_outside(own, halo, member, beams, SET)
    bases = [0, 1, 2, 3]
    merge_level(own, halo, 2, bases, member, beams, sources, merge_ref.at[2], shift_ref, last)


def image_kernel(groups, beams_ref, *rest):
    maps, out_ref = rest[:SET], rest[SET]
    own = beams_ref.shape[2]
    width = maps[0].shape[1]
    piece = out_ref.shape[2]
    for half in range(2):
        total = jnp.zeros((own, width), jnp.float32)
        for slot in range(SET):
            real, imag = beams_ref[slot, 0], beams_ref[slot, 1]
            left = jnp.concatenate([real, -imag] if half == 0 else [imag, real], axis=1)
            total += jnp.dot(left, maps[slot][...], preferred_element_type=jnp.float32)
        total = total.astype(jnp.bfloat16)
        for at in range(own // piece):
            out_ref[at % groups, at // groups, :, half * width : (half + 1) * width] = total[
                at * piece : (at + 1) * piece
            ]


def sum_kernel(pieces_ref, out_ref):
    total = pieces_ref[0].astype(jnp.float32)
    for source in range(1, pieces_ref.shape[0]):
        total += pieces_ref[source].astype(jnp.float32)
    total = total.astype(jnp.bfloat16)
    out_ref[0] = total
    out_ref[1] = total


def last_kernel(half_ref, pieces_ref, out_ref):
    many = pieces_ref.shape[0] // 2
    base = half_ref[0] * many
    total = pieces_ref[base].astype(jnp.float32)
    for source in range(1, many):
        total += pieces_ref[base + source].astype(jnp.float32)
    out_ref[...] = total


def call(kernel, name, out_shape, in_specs, scratch=(), flops=0, vmem=24, out_specs=None):
    return pl.pallas_call(
        kernel,
        out_shape=out_shape,
        in_specs=in_specs,
        out_specs=jax.tree.map(lambda _: VMEM, out_shape) if out_specs is None else out_specs,
        scratch_shapes=scratch,
        cost_estimate=pl.CostEstimate(flops=flops, bytes_accessed=2**20, transcendentals=0),
        compiler_params=pltpu.CompilerParams(vmem_limit_bytes=vmem * 2**20),
        name=name,
    )


def body(pulses, steering, merge_re, merge_im, range_shift, image_map):
    total_rows = pulses.shape[0]
    count = steering.shape[2]
    levels = merge_re.shape[0]
    groups = lax.axis_size("pulse")
    tiles = lax.axis_size("tile")
    sets = tiles // SET
    own = total_rows // SET
    halo = levels * SHIFT
    rows = own + 2 * halo
    piece = own // tiles
    half_type = jnp.bfloat16
    member = lax.axis_index("tile") % SET
    where = member.reshape(1).astype(jnp.int32)

    def swap(value, mask):
        return lax.ppermute(value, "tile", [(s, s ^ mask) for s in range(tiles)])

    raw = pulses.reshape(2 * total_rows, count)
    windows = call(
        functools.partial(windows_kernel, own, halo),
        "windows",
        [jax.ShapeDtypeStruct((2 * rows, count), half_type)] * SET,
        [SMEM, pl.BlockSpec(memory_space=pltpu.HBM)],
        scratch=[pltpu.SemaphoreType.DMA((SET, 3))],
    )(where, raw)
    arrived = {0: windows[0]}
    for mask in (4, 2, 5, 3, 1, 6, 7):
        arrived[mask] = swap(windows[mask], mask)

    own_map = image_map.reshape(2 * count, -1)
    width = own_map.shape[1]
    held = {0: own_map}
    for mask in (4, 2, 6):
        held[mask] = swap(own_map, mask)
    for slot in (0, 4, 2, 6):
        held[slot | 1] = swap(held[slot], 1)

    steer_block, merge_block = call(
        weights_kernel,
        "weights",
        [
            jax.ShapeDtypeStruct((2 * count, 2 * count), half_type),
            jax.ShapeDtypeStruct((levels, 4 * count, 4 * count), half_type),
        ],
        [VMEM] * 3,
        flops=10**8,
    )(steering, merge_re, merge_im)

    started = []
    for base in range(0, SET, 2):
        started.append(
            call(
                functools.partial(start_kernel, own, halo),
                "start",
                jax.ShapeDtypeStruct((2, 2, rows + 2 * SHIFT, count), half_type),
                [SMEM] + [VMEM] * 5,
                scratch=[
                    pltpu.VMEM((2, 2, rows + 2 * SHIFT, count), half_type),
                    pltpu.VMEM((rows, 4 * count), half_type),
                    pltpu.VMEM((2 * rows, count), jnp.float32),
                ],
                flops=5 * 10**8,
            )(where, arrived[base], arrived[base + 1], steer_block, merge_block, range_shift)
        )
    beams = call(
        functools.partial(finish_kernel, own, halo),
        "finish",
        jax.ShapeDtypeStruct((SET, 2, own, count), half_type),
        [SMEM] + [VMEM] * (SET // 2 + 2),
        scratch=[
            pltpu.VMEM((SET, 2, rows + 2 * SHIFT, count), half_type),
            pltpu.VMEM((rows, 4 * count), half_type),
        ],
        flops=25 * 10**8,
    )(where, *started, merge_block, range_shift)
    partial_rows = call(
        functools.partial(image_kernel, groups),
        "image",
        jax.ShapeDtypeStruct((groups, sets, piece, 2 * width), half_type),
        [VMEM] * (1 + SET),
        flops=2 * 10**9,
    )(beams, *[held[slot] for slot in range(SET)])

    pieces = lax.all_to_all(partial_rows, "pulse", 0, 0, tiled=True)
    doubled = call(
        sum_kernel, "sum", jax.ShapeDtypeStruct((2, sets, piece, 2 * width), half_type), [VMEM]
    )(pieces)

    def device(pulse, u, i):
        return pulse * tiles + u * SET + i

    crossing = []
    for a in range(groups):
        for b in range(a + 1, groups):
            crossing.append(
                [device(a, u, b) for u in range(sets)] + [device(b, u, a) for u in range(sets)]
            )
    for a in range(0, groups, 2):
        crossing.append(
            [device(a, u, a) for u in range(sets)] + [device(a + 1, u, a + 1) for u in range(sets)]
        )
    last = lax.all_to_all(
        doubled.reshape(2 * sets, piece, 2 * width),
        ("pulse", "tile"),
        0,
        0,
        axis_index_groups=crossing,
        tiled=True,
    )
    pulse = lax.axis_index("pulse")
    half = jnp.where(pulse == member, pulse % 2, (pulse < member).astype(jnp.int32))
    return call(
        last_kernel, "last", jax.ShapeDtypeStruct((piece, 2 * width), jnp.float32), [SMEM, VMEM]
    )(half.reshape(1).astype(jnp.int32), last)


def solution(mesh):
    placed = (
        P(None, None, ("pulse", "tile")),
        P(),
        P(),
        P(),
        P(),
        P("pulse", "tile", None, None, None),
    )
    return jax.shard_map(
        body, mesh=mesh, in_specs=placed, out_specs=P(("pulse", "tile"), None), check_vma=False
    )
```

```python
import functools

import jax
import jax.numpy as jnp
from jax import lax
from jax.experimental import pallas as pl
from jax.experimental.pallas import tpu as pltpu
from jax.sharding import PartitionSpec as P


SHIFT = 8
SET = 8
VMEM = pl.BlockSpec(memory_space=pltpu.VMEM)
SMEM = pl.BlockSpec(memory_space=pltpu.SMEM)


def swapped(index):
    return ((index >> 1) & 1) << 2 | ((index >> 2) & 1) << 1 | (index & 1)


def weights_kernel(steering_ref, merge_re_ref, merge_im_ref, steer_ref, merge_ref):
    def block(out, real, imag):
        high, wide = real.shape
        out[:high, :wide] = real
        out[:high, wide:] = imag
        out[high:, :wide] = -imag
        out[high:, wide:] = real

    block(steer_ref, steering_ref[0], steering_ref[1])
    for level in range(merge_re_ref.shape[0]):
        block(merge_ref.at[level], merge_re_ref[level], merge_im_ref[level])


def windows_kernel(own, halo, member_ref, raw_ref, *rest):
    outs, sems = rest[:SET], rest[SET]
    member = member_ref[0]
    main, edge = 2 * own, 2 * halo

    def copy(slot, kind, source, target, length):
        return pltpu.make_async_copy(
            raw_ref.at[pl.ds(pl.multiple_of(source, 16), length), :],
            outs[slot].at[pl.ds(target, length), :],
            sems.at[slot, kind],
        )

    def each(action):
        for slot in range(SET):
            block = swapped(member ^ slot)
            start = block * main
            action(copy(slot, 0, start, edge, main))

            @pl.when(block > 0)
            def _():
                action(copy(slot, 1, start - edge, 0, edge))

            @pl.when(block < SET - 1)
            def _():
                action(copy(slot, 2, start + main, edge + main, edge))

    each(lambda made: made.start())
    zeros = jnp.zeros((edge, raw_ref.shape[1]), raw_ref.dtype)
    for slot in range(SET):
        block = swapped(member ^ slot)

        @pl.when(block == 0)
        def _():
            outs[slot][:edge, :] = zeros

        @pl.when(block == SET - 1)
        def _():
            outs[slot][edge + main :, :] = zeros

    each(lambda made: made.wait())


def moved_rows(beams, slot, part, pick, before, after, base, chunk):
    value = beams[slot, part, pl.ds(base, chunk + 2 * SHIFT), :].astype(jnp.float32)
    turned = [
        jnp.take_along_axis(value[tile * SHIFT : (tile + 1) * SHIFT], pick, axis=0)
        for tile in range(chunk // SHIFT + 2)
    ]
    moved = [
        jnp.where(before, turned[tile], jnp.where(after, turned[tile + 2], turned[tile + 1]))
        for tile in range(chunk // SHIFT)
    ]
    return jnp.concatenate(moved, axis=0).astype(jnp.bfloat16)


def merge_level(own, halo, level, base_slots, member, beams, sources, merge, shift_ref, emit):
    count = beams.shape[-1]
    rows = own + 2 * halo
    chunk = 80
    sublane = lax.broadcasted_iota(jnp.int32, (SHIFT, count), 0)
    picks, befores, afters = [], [], []
    for side in range(2):
        offset = jnp.broadcast_to(shift_ref[level, side : side + 1, :], (SHIFT, count)) + sublane
        picks.append(offset & (SHIFT - 1))
        befores.append(offset < 0)
        afters.append(offset >= SHIFT)
    bit = (member >> level) & 1

    def pair(base):
        ends = (base + (bit << level), base + ((1 - bit) << level))

        def shift(step, carry):
            at = pl.multiple_of(step * chunk, 16)
            for side in range(2):
                for part in range(2):
                    column = (2 * part + side) * count
                    sources[pl.ds(at, chunk), column : column + count] = moved_rows(
                        beams, ends[side], part, picks[side], befores[side], afters[side], at, chunk
                    )
            return carry

        lax.fori_loop(0, rows // chunk, shift, 0)
        for part in range(2):
            result = jnp.dot(
                sources[...],
                merge[:, 2 * part * count : 2 * (part + 1) * count],
                preferred_element_type=jnp.float32,
            ).astype(jnp.bfloat16)
            for side in range(2):
                emit(ends[side], part, result[:, side * count : (side + 1) * count])

    if len(base_slots) == 1:
        pair(base_slots[0])
    else:
        def step(index, carry):
            low = ((index >> level) << (level + 1)) | (index & (2**level - 1))
            pair(low)
            return carry

        lax.fori_loop(0, len(base_slots), step, 0)


def start_kernel(own, halo, member_ref, left_ref, right_ref, steer_ref, merge_ref, shift_ref, out_ref,
                 beams, sources, spread):
    count = steer_ref.shape[1] // 2
    rows = own + 2 * halo
    member = member_ref[0]
    zeros = jnp.zeros((SHIFT, count), jnp.bfloat16)
    for slot, raw_ref in enumerate((left_ref, right_ref)):
        for part in range(2):
            beams[slot, part, :SHIFT, :] = zeros
            beams[slot, part, SHIFT + rows :, :] = zeros
            out_ref[slot, part, :SHIFT, :] = zeros
            out_ref[slot, part, SHIFT + rows :, :] = zeros
        spread[...] = raw_ref[...].astype(jnp.float32)
        real = spread[pl.ds(0, rows, stride=2), :].astype(jnp.bfloat16)
        imag = spread[pl.ds(1, rows, stride=2), :].astype(jnp.bfloat16)
        result = jnp.dot(
            jnp.concatenate([real, imag], axis=1), steer_ref[...], preferred_element_type=jnp.float32
        ).astype(jnp.bfloat16)
        beams[slot, 0, pl.ds(SHIFT, rows), :] = result[:, :count]
        beams[slot, 1, pl.ds(SHIFT, rows), :] = result[:, count:]

    def emit(slot, part, value):
        out_ref[slot, part, pl.ds(SHIFT, rows), :] = value

    merge_level(own, halo, 0, [0], member, beams, sources, merge_ref.at[0], shift_ref, emit)
    clear_outside(own, halo, member, out_ref, 2)


def clear_outside(own, halo, member, beams, slots):
    zeros = jnp.zeros((halo, beams.shape[-1]), beams.dtype)

    @pl.when(member == 0)
    def _():
        for slot in range(slots):
            for part in range(2):
                beams[slot, part, SHIFT : SHIFT + halo, :] = zeros

    @pl.when(member == SET - 1)
    def _():
        for slot in range(slots):
            for part in range(2):
                beams[slot, part, SHIFT + halo + own : SHIFT + 2 * halo + own, :] = zeros


def middle_kernel(own, halo, member_ref, left_ref, right_ref, merge_ref, shift_ref, out_ref, beams, sources):
    count = beams.shape[-1]
    rows = own + 2 * halo
    member = member_ref[0]
    beams[0:2] = left_ref[...]
    beams[2:4] = right_ref[...]
    zeros = jnp.zeros((SHIFT, count), jnp.bfloat16)
    for slot in range(SET // 2):
        for part in range(2):
            out_ref[slot, part, :SHIFT, :] = zeros
            out_ref[slot, part, SHIFT + rows :, :] = zeros

    def emit(slot, part, value):
        out_ref[slot, part, pl.ds(SHIFT, rows), :] = value

    merge_level(own, halo, 1, [0, 1], member, beams, sources, merge_ref.at[1], shift_ref, emit)
    clear_outside(own, halo, member, out_ref, SET // 2)


def finish_kernel(
    own, halo, member_ref, middle_ref, left_ref, right_ref, merge_ref, shift_ref, out_ref, beams, sources
):
    rows = own + 2 * halo
    member = member_ref[0]
    high = beams.at[SET // 2 :]
    beams[: SET // 2] = middle_ref[...]
    high[0:2] = left_ref[...]
    high[2:4] = right_ref[...]

    def keep(slot, part, value):
        high[slot, part, pl.ds(SHIFT, rows), :] = value

    def last(slot, part, value):
        out_ref[slot, part] = value[halo : halo + own]

    merge_level(own, halo, 1, [0, 1], member, high, sources, merge_ref.at[1], shift_ref, keep)
    clear_outside(own, halo, member, high, SET // 2)
    merge_level(own, halo, 2, [0, 1, 2, 3], member, beams, sources, merge_ref.at[2], shift_ref, last)


def image_kernel(groups, beams_ref, *rest):
    maps, out_ref = rest[:SET], rest[SET]
    own = beams_ref.shape[2]
    width = maps[0].shape[1]
    piece = out_ref.shape[2]
    for half in range(2):
        total = jnp.zeros((own, width), jnp.float32)
        for slot in range(SET):
            real, imag = beams_ref[slot, 0], beams_ref[slot, 1]
            left = jnp.concatenate([real, -imag] if half == 0 else [imag, real], axis=1)
            total += jnp.dot(left, maps[slot][...], preferred_element_type=jnp.float32)
        total = total.astype(jnp.bfloat16)
        for at in range(own // piece):
            out_ref[swapped(at % groups), at // groups, :, half * width : (half + 1) * width] = total[
                at * piece : (at + 1) * piece
            ]


def sum_kernel(pieces_ref, out_ref):
    total = pieces_ref[0].astype(jnp.float32)
    for source in range(1, pieces_ref.shape[0]):
        total += pieces_ref[source].astype(jnp.float32)
    total = total.astype(jnp.bfloat16)
    out_ref[0] = total
    out_ref[1] = total


def last_kernel(half_ref, pieces_ref, out_ref):
    many = pieces_ref.shape[0] // 2
    base = half_ref[0] * many
    total = pieces_ref[base].astype(jnp.float32)
    for source in range(1, many):
        total += pieces_ref[base + source].astype(jnp.float32)
    out_ref[...] = total


def call(kernel, out_shape, in_specs, scratch=(), flops=0, vmem=24, out_specs=None):
    def run(*operands):
        return called(kernel, out_shape, in_specs, scratch, flops, vmem, out_specs)(*operands)

    return run


def called(kernel, out_shape, in_specs, scratch, flops, vmem, out_specs):
    return pl.pallas_call(
        kernel,
        out_shape=out_shape,
        in_specs=in_specs,
        out_specs=jax.tree.map(lambda _: VMEM, out_shape) if out_specs is None else out_specs,
        scratch_shapes=scratch,
        cost_estimate=pl.CostEstimate(flops=flops, bytes_accessed=2**20, transcendentals=0),
        compiler_params=pltpu.CompilerParams(vmem_limit_bytes=vmem * 2**20),
    )


def body(pulses, steering, merge_re, merge_im, range_shift, image_map):
    total_rows = pulses.shape[0]
    count = steering.shape[2]
    levels = merge_re.shape[0]
    groups = lax.axis_size("pulse")
    tiles = lax.axis_size("tile")
    sets = tiles // SET
    own = total_rows // SET
    halo = levels * SHIFT
    rows = own + 2 * halo
    piece = own // tiles
    half_type = jnp.bfloat16
    member = lax.axis_index("tile") % SET
    where = member.reshape(1).astype(jnp.int32)

    def swap(value, mask):
        return lax.ppermute(value, "tile", [(s, s ^ mask) for s in range(tiles)])

    raw = pulses.reshape(2 * total_rows, count)
    windows = call(
        functools.partial(windows_kernel, own, halo),
        [jax.ShapeDtypeStruct((2 * rows, count), half_type)] * SET,
        [SMEM, pl.BlockSpec(memory_space=pltpu.HBM)],
        scratch=[pltpu.SemaphoreType.DMA((SET, 3))],
        vmem=60,
    )(where, raw)
    arrived = {0: windows[0]}
    for mask in (4, 2, 5, 3, 1, 6, 7):
        arrived[mask] = swap(windows[mask], mask)

    own_map = image_map.reshape(2 * count, -1)
    width = own_map.shape[1]
    held = {0: own_map}
    for mask in (4, 2, 6):
        held[mask] = swap(own_map, mask)
    for slot in (0, 4, 2, 6):
        held[slot | 1] = swap(held[slot], 1)

    steer_block, merge_block = call(
        weights_kernel,
        [
            jax.ShapeDtypeStruct((2 * count, 2 * count), half_type),
            jax.ShapeDtypeStruct((levels, 4 * count, 4 * count), half_type),
        ],
        [VMEM] * 3,
        flops=10**8,
    )(steering, merge_re, merge_im)

    started = []
    for base in range(0, SET, 2):
        started.append(
            call(
                functools.partial(start_kernel, own, halo),
                jax.ShapeDtypeStruct((2, 2, rows + 2 * SHIFT, count), half_type),
                [SMEM] + [VMEM] * 5,
                scratch=[
                    pltpu.VMEM((2, 2, rows + 2 * SHIFT, count), half_type),
                    pltpu.VMEM((rows, 4 * count), half_type),
                    pltpu.VMEM((2 * rows, count), jnp.float32),
                ],
                flops=5 * 10**8,
            )(where, arrived[base], arrived[base + 1], steer_block, merge_block, range_shift)
        )
    middle = call(
        functools.partial(middle_kernel, own, halo),
        jax.ShapeDtypeStruct((SET // 2, 2, rows + 2 * SHIFT, count), half_type),
        [SMEM] + [VMEM] * 4,
        scratch=[
            pltpu.VMEM((SET // 2, 2, rows + 2 * SHIFT, count), half_type),
            pltpu.VMEM((rows, 4 * count), half_type),
        ],
        flops=6 * 10**8,
    )(where, started[0], started[1], merge_block, range_shift)
    beams = call(
        functools.partial(finish_kernel, own, halo),
        jax.ShapeDtypeStruct((SET, 2, own, count), half_type),
        [SMEM] + [VMEM] * 5,
        scratch=[
            pltpu.VMEM((SET, 2, rows + 2 * SHIFT, count), half_type),
            pltpu.VMEM((rows, 4 * count), half_type),
        ],
        flops=18 * 10**8,
    )(where, middle, started[2], started[3], merge_block, range_shift)
    partial_rows = call(
        functools.partial(image_kernel, groups),
        jax.ShapeDtypeStruct((groups, sets, piece, 2 * width), half_type),
        [VMEM] * (1 + SET),
        flops=2 * 10**9,
    )(beams, *[held[slot] for slot in range(SET)])

    pieces = lax.all_to_all(partial_rows, "pulse", 0, 0, tiled=True)
    doubled = call(
        sum_kernel, jax.ShapeDtypeStruct((2, sets, piece, 2 * width), half_type), [VMEM]
    )(pieces)

    def device(pulse, u, i):
        return pulse * tiles + u * SET + swapped(i)

    crossing = []
    for a in range(groups):
        for b in range(a + 1, groups):
            crossing.append(
                [device(a, u, b) for u in range(sets)] + [device(b, u, a) for u in range(sets)]
            )
    for a in range(0, groups, 2):
        crossing.append(
            [device(a, u, a) for u in range(sets)] + [device(a + 1, u, a + 1) for u in range(sets)]
        )
    last = lax.all_to_all(
        doubled.reshape(2 * sets, piece, 2 * width),
        ("pulse", "tile"),
        0,
        0,
        axis_index_groups=crossing,
        tiled=True,
    )
    pulse = lax.axis_index("pulse")
    target = swapped(member)
    half = jnp.where(pulse == target, pulse % 2, (pulse < target).astype(jnp.int32))
    return call(
        last_kernel, jax.ShapeDtypeStruct((piece, 2 * width), jnp.float32), [SMEM, VMEM]
    )(half.reshape(1).astype(jnp.int32), last)


def solution(mesh):
    placed = (
        P(None, None, ("pulse", "tile")),
        P(),
        P(),
        P(),
        P(),
        P("pulse", "tile", None, None, None),
    )
    return jax.shard_map(
        body, mesh=mesh, in_specs=placed, out_specs=P(("pulse", "tile"), None), check_vma=False
    )
```

```python
import functools

import jax
import jax.numpy as jnp
from jax import lax
from jax.experimental import pallas as pl
from jax.experimental.pallas import tpu as pltpu
from jax.sharding import PartitionSpec as P


SHIFT = 8
SET = 8
VMEM = pl.BlockSpec(memory_space=pltpu.VMEM)
SMEM = pl.BlockSpec(memory_space=pltpu.SMEM)


def swapped(index):
    return ((index >> 1) & 1) << 2 | ((index >> 2) & 1) << 1 | (index & 1)


def weights_kernel(steering_ref, merge_re_ref, merge_im_ref, steer_ref, merge_ref):
    def block(out, real, imag):
        high, wide = real.shape
        out[:high, :wide] = real
        out[:high, wide:] = imag
        out[high:, :wide] = -imag
        out[high:, wide:] = real

    block(steer_ref, steering_ref[0], steering_ref[1])
    for level in range(merge_re_ref.shape[0]):
        block(merge_ref.at[level], merge_re_ref[level], merge_im_ref[level])


def windows_kernel(own, halo, member_ref, raw_ref, *rest):
    outs, sems = rest[:SET], rest[SET]
    member = member_ref[0]
    main, edge = 2 * own, 2 * halo

    def copy(slot, kind, source, target, length):
        return pltpu.make_async_copy(
            raw_ref.at[pl.ds(pl.multiple_of(source, 16), length), :],
            outs[slot].at[pl.ds(target, length), :],
            sems.at[slot, kind],
        )

    def each(action):
        for slot in range(SET):
            block = swapped(member ^ slot)
            start = block * main
            action(copy(slot, 0, start, edge, main))

            @pl.when(block > 0)
            def _():
                action(copy(slot, 1, start - edge, 0, edge))

            @pl.when(block < SET - 1)
            def _():
                action(copy(slot, 2, start + main, edge + main, edge))

    each(lambda made: made.start())
    zeros = jnp.zeros((edge, raw_ref.shape[1]), raw_ref.dtype)
    for slot in range(SET):
        block = swapped(member ^ slot)

        @pl.when(block == 0)
        def _():
            outs[slot][:edge, :] = zeros

        @pl.when(block == SET - 1)
        def _():
            outs[slot][edge + main :, :] = zeros

    each(lambda made: made.wait())


def moved_rows(beams, slot, part, pick, before, after, base, chunk):
    value = beams[slot, part, pl.ds(base, chunk + 2 * SHIFT), :].astype(jnp.float32)
    turned = [
        jnp.take_along_axis(value[tile * SHIFT : (tile + 1) * SHIFT], pick, axis=0)
        for tile in range(chunk // SHIFT + 2)
    ]
    moved = [
        jnp.where(before, turned[tile], jnp.where(after, turned[tile + 2], turned[tile + 1]))
        for tile in range(chunk // SHIFT)
    ]
    return jnp.concatenate(moved, axis=0).astype(jnp.bfloat16)


def merge_level(own, halo, level, base_slots, member, beams, sources, merge, shift_ref, emit):
    count = beams.shape[-1]
    rows = own + 2 * halo
    chunk = 80
    sublane = lax.broadcasted_iota(jnp.int32, (SHIFT, count), 0)
    picks, befores, afters = [], [], []
    for side in range(2):
        offset = jnp.broadcast_to(shift_ref[level, side : side + 1, :], (SHIFT, count)) + sublane
        picks.append(offset & (SHIFT - 1))
        befores.append(offset < 0)
        afters.append(offset >= SHIFT)
    bit = (member >> level) & 1

    def pair(base):
        ends = (base + (bit << level), base + ((1 - bit) << level))

        def shift(step, carry):
            at = pl.multiple_of(step * chunk, 16)
            for side in range(2):
                for part in range(2):
                    column = (2 * part + side) * count
                    sources[pl.ds(at, chunk), column : column + count] = moved_rows(
                        beams, ends[side], part, picks[side], befores[side], afters[side], at, chunk
                    )
            return carry

        lax.fori_loop(0, rows // chunk, shift, 0)
        for part in range(2):
            result = jnp.dot(
                sources[...],
                merge[:, 2 * part * count : 2 * (part + 1) * count],
                preferred_element_type=jnp.float32,
            ).astype(jnp.bfloat16)
            for side in range(2):
                emit(ends[side], part, result[:, side * count : (side + 1) * count])

    if len(base_slots) == 1:
        pair(base_slots[0])
    else:
        def step(index, carry):
            low = ((index >> level) << (level + 1)) | (index & (2**level - 1))
            pair(low)
            return carry

        lax.fori_loop(0, len(base_slots), step, 0)


def start_kernel(own, halo, member_ref, left_ref, right_ref, steer_ref, merge_ref, shift_ref, out_ref,
                 beams, sources, spread):
    count = steer_ref.shape[1] // 2
    rows = own + 2 * halo
    member = member_ref[0]
    zeros = jnp.zeros((SHIFT, count), jnp.bfloat16)
    for slot, raw_ref in enumerate((left_ref, right_ref)):
        for part in range(2):
            beams[slot, part, :SHIFT, :] = zeros
            beams[slot, part, SHIFT + rows :, :] = zeros
            out_ref[slot, part, :SHIFT, :] = zeros
            out_ref[slot, part, SHIFT + rows :, :] = zeros
        spread[...] = raw_ref[...].astype(jnp.float32)
        real = spread[pl.ds(0, rows, stride=2), :].astype(jnp.bfloat16)
        imag = spread[pl.ds(1, rows, stride=2), :].astype(jnp.bfloat16)
        result = jnp.dot(
            jnp.concatenate([real, imag], axis=1), steer_ref[...], preferred_element_type=jnp.float32
        ).astype(jnp.bfloat16)
        beams[slot, 0, pl.ds(SHIFT, rows), :] = result[:, :count]
        beams[slot, 1, pl.ds(SHIFT, rows), :] = result[:, count:]

    def emit(slot, part, value):
        out_ref[slot, part, pl.ds(SHIFT, rows), :] = value

    merge_level(own, halo, 0, [0], member, beams, sources, merge_ref.at[0], shift_ref, emit)
    clear_outside(own, halo, member, out_ref, 2)


def clear_outside(own, halo, member, beams, slots):
    zeros = jnp.zeros((halo, beams.shape[-1]), beams.dtype)

    @pl.when(member == 0)
    def _():
        for slot in range(slots):
            for part in range(2):
                beams[slot, part, SHIFT : SHIFT + halo, :] = zeros

    @pl.when(member == SET - 1)
    def _():
        for slot in range(slots):
            for part in range(2):
                beams[slot, part, SHIFT + halo + own : SHIFT + 2 * halo + own, :] = zeros


def middle_kernel(own, halo, member_ref, left_ref, right_ref, merge_ref, shift_ref, out_ref, beams, sources):
    count = beams.shape[-1]
    rows = own + 2 * halo
    member = member_ref[0]
    beams[0:2] = left_ref[...]
    beams[2:4] = right_ref[...]
    zeros = jnp.zeros((SHIFT, count), jnp.bfloat16)
    for slot in range(SET // 2):
        for part in range(2):
            out_ref[slot, part, :SHIFT, :] = zeros
            out_ref[slot, part, SHIFT + rows :, :] = zeros

    def emit(slot, part, value):
        out_ref[slot, part, pl.ds(SHIFT, rows), :] = value

    merge_level(own, halo, 1, [0, 1], member, beams, sources, merge_ref.at[1], shift_ref, emit)
    clear_outside(own, halo, member, out_ref, SET // 2)


def finish_kernel(
    own, halo, member_ref, middle_ref, left_ref, right_ref, merge_ref, shift_ref, out_ref, beams, sources
):
    rows = own + 2 * halo
    member = member_ref[0]
    high = beams.at[SET // 2 :]
    beams[: SET // 2] = middle_ref[...]
    high[0:2] = left_ref[...]
    high[2:4] = right_ref[...]

    def keep(slot, part, value):
        high[slot, part, pl.ds(SHIFT, rows), :] = value

    def last(slot, part, value):
        out_ref[slot, part] = value[halo : halo + own]

    merge_level(own, halo, 1, [0, 1], member, high, sources, merge_ref.at[1], shift_ref, keep)
    clear_outside(own, halo, member, high, SET // 2)
    merge_level(own, halo, 2, [0, 1, 2, 3], member, beams, sources, merge_ref.at[2], shift_ref, last)


def image_kernel(groups, beams_ref, *rest):
    maps, halves, out_ref = rest[: SET - 2], rest[SET - 2 : SET + 2], rest[SET + 2]
    own = beams_ref.shape[2]
    width = maps[0].shape[1]
    values = [ref[...] for ref in maps] + [
        jnp.concatenate([halves[at][...], halves[at + 1][...]], axis=0) for at in (0, 2)
    ]
    piece = out_ref.shape[2]
    for half in range(2):
        total = jnp.zeros((own, width), jnp.float32)
        for slot in range(SET):
            real, imag = beams_ref[slot, 0], beams_ref[slot, 1]
            left = jnp.concatenate([real, -imag] if half == 0 else [imag, real], axis=1)
            total += jnp.dot(left, values[slot], preferred_element_type=jnp.float32)
        total = total.astype(jnp.bfloat16)
        for at in range(own // piece):
            out_ref[swapped(at % groups), at // groups, :, half * width : (half + 1) * width] = total[
                at * piece : (at + 1) * piece
            ]


def sum_kernel(pieces_ref, out_ref):
    total = pieces_ref[0].astype(jnp.float32)
    for source in range(1, pieces_ref.shape[0]):
        total += pieces_ref[source].astype(jnp.float32)
    total = total.astype(jnp.bfloat16)
    out_ref[0] = total
    out_ref[1] = total


def last_kernel(half_ref, pieces_ref, out_ref):
    many = pieces_ref.shape[0] // 2
    base = half_ref[0] * many
    total = pieces_ref[base].astype(jnp.float32)
    for source in range(1, many):
        total += pieces_ref[base + source].astype(jnp.float32)
    out_ref[...] = total


def call(kernel, out_shape, in_specs, scratch=(), flops=0, vmem=24, out_specs=None):
    def run(*operands):
        return called(kernel, out_shape, in_specs, scratch, flops, vmem, out_specs)(*operands)

    return run


def called(kernel, out_shape, in_specs, scratch, flops, vmem, out_specs):
    return pl.pallas_call(
        kernel,
        out_shape=out_shape,
        in_specs=in_specs,
        out_specs=jax.tree.map(lambda _: VMEM, out_shape) if out_specs is None else out_specs,
        scratch_shapes=scratch,
        cost_estimate=pl.CostEstimate(flops=flops, bytes_accessed=2**20, transcendentals=0),
        compiler_params=pltpu.CompilerParams(vmem_limit_bytes=vmem * 2**20),
    )


def body(pulses, steering, merge_re, merge_im, range_shift, image_map):
    total_rows = pulses.shape[0]
    count = steering.shape[2]
    levels = merge_re.shape[0]
    groups = lax.axis_size("pulse")
    tiles = lax.axis_size("tile")
    sets = tiles // SET
    own = total_rows // SET
    halo = levels * SHIFT
    rows = own + 2 * halo
    piece = own // tiles
    half_type = jnp.bfloat16
    member = lax.axis_index("tile") % SET
    where = member.reshape(1).astype(jnp.int32)

    def swap(value, mask):
        return lax.ppermute(value, "tile", [(s, s ^ mask) for s in range(tiles)])

    raw = pulses.reshape(2 * total_rows, count)
    windows = call(
        functools.partial(windows_kernel, own, halo),
        [jax.ShapeDtypeStruct((2 * rows, count), half_type)] * SET,
        [SMEM, pl.BlockSpec(memory_space=pltpu.HBM)],
        scratch=[pltpu.SemaphoreType.DMA((SET, 3))],
    )(where, raw)
    arrived = {0: windows[0]}
    for mask in (4, 2, 5, 3, 1, 6, 7):
        arrived[mask] = swap(windows[mask], mask)

    own_map = image_map.reshape(2 * count, -1)
    width = own_map.shape[1]
    held = {0: own_map}
    for mask in (2, 4):
        held[mask] = swap(own_map, mask)
    for slot in (0, 2, 4):
        held[slot | 1] = swap(held[slot], 1)
    far = (swap(held[4][:count], 2), swap(held[2][count:], 4))
    near = (swap(far[0], 1), swap(far[1], 1))

    steer_block, merge_block = call(
        weights_kernel,
        [
            jax.ShapeDtypeStruct((2 * count, 2 * count), half_type),
            jax.ShapeDtypeStruct((levels, 4 * count, 4 * count), half_type),
        ],
        [VMEM] * 3,
        flops=10**8,
    )(steering, merge_re, merge_im)

    started = []
    for base in range(0, SET, 2):
        started.append(
            call(
                functools.partial(start_kernel, own, halo),
                jax.ShapeDtypeStruct((2, 2, rows + 2 * SHIFT, count), half_type),
                [SMEM] + [VMEM] * 5,
                scratch=[
                    pltpu.VMEM((2, 2, rows + 2 * SHIFT, count), half_type),
                    pltpu.VMEM((rows, 4 * count), half_type),
                    pltpu.VMEM((2 * rows, count), jnp.float32),
                ],
                flops=5 * 10**8,
            )(where, arrived[base], arrived[base + 1], steer_block, merge_block, range_shift)
        )
    middle = call(
        functools.partial(middle_kernel, own, halo),
        jax.ShapeDtypeStruct((SET // 2, 2, rows + 2 * SHIFT, count), half_type),
        [SMEM] + [VMEM] * 4,
        scratch=[
            pltpu.VMEM((SET // 2, 2, rows + 2 * SHIFT, count), half_type),
            pltpu.VMEM((rows, 4 * count), half_type),
        ],
        flops=6 * 10**8,
    )(where, started[0], started[1], merge_block, range_shift)
    beams = call(
        functools.partial(finish_kernel, own, halo),
        jax.ShapeDtypeStruct((SET, 2, own, count), half_type),
        [SMEM] + [VMEM] * 5,
        scratch=[
            pltpu.VMEM((SET, 2, rows + 2 * SHIFT, count), half_type),
            pltpu.VMEM((rows, 4 * count), half_type),
        ],
        flops=18 * 10**8,
    )(where, middle, started[2], started[3], merge_block, range_shift)
    partial_rows = call(
        functools.partial(image_kernel, groups),
        jax.ShapeDtypeStruct((groups, sets, piece, 2 * width), half_type),
        [VMEM] * (3 + SET),
        flops=2 * 10**9,
    )(beams, *[held[slot] for slot in range(SET - 2)], *far, *near)

    pieces = lax.all_to_all(partial_rows, "pulse", 0, 0, tiled=True)
    doubled = call(sum_kernel, jax.ShapeDtypeStruct((2, sets, piece, 2 * width), half_type), [VMEM])(pieces)

    def device(pulse, u, i):
        return pulse * tiles + u * SET + swapped(i)

    crossing = []
    for a in range(groups):
        for b in range(a + 1, groups):
            crossing.append(
                [device(a, u, b) for u in range(sets)] + [device(b, u, a) for u in range(sets)]
            )
    for a in range(0, groups, 2):
        crossing.append(
            [device(a, u, a) for u in range(sets)] + [device(a + 1, u, a + 1) for u in range(sets)]
        )
    last = lax.all_to_all(
        doubled.reshape(2 * sets, piece, 2 * width),
        ("pulse", "tile"),
        0,
        0,
        axis_index_groups=crossing,
        tiled=True,
    )
    pulse = lax.axis_index("pulse")
    target = swapped(member)
    half = jnp.where(pulse == target, pulse % 2, (pulse < target).astype(jnp.int32))
    return call(
        last_kernel, jax.ShapeDtypeStruct((piece, 2 * width), jnp.float32), [SMEM, VMEM]
    )(half.reshape(1).astype(jnp.int32), last)


def solution(mesh):
    placed = (
        P(None, None, ("pulse", "tile")),
        P(),
        P(),
        P(),
        P(),
        P("pulse", "tile", None, None, None),
    )
    return jax.shard_map(
        body, mesh=mesh, in_specs=placed, out_specs=P(("pulse", "tile"), None), check_vma=False
    )
```

```python
import functools

import jax
import jax.numpy as jnp
from jax import lax
from jax.experimental import pallas as pl
from jax.experimental.pallas import tpu as pltpu
from jax.sharding import PartitionSpec as P


SHIFT = 8
SET = 8
VMEM = pl.BlockSpec(memory_space=pltpu.VMEM)
SMEM = pl.BlockSpec(memory_space=pltpu.SMEM)


def swapped(index):
    return ((index >> 1) & 1) << 2 | ((index >> 2) & 1) << 1 | (index & 1)


def weights_kernel(member_ref, steering_ref, merge_re_ref, merge_im_ref, steer_ref, merge_ref):
    def block(out, real, imag):
        high, wide = real.shape
        out[:high, :wide] = real
        out[:high, wide:] = imag
        out[high:, :wide] = -imag
        out[high:, wide:] = real

    def arranged(matrix, bit):
        count = matrix.shape[0] // 2
        turned = jnp.concatenate([matrix[count:], matrix[:count]], axis=0)
        turned = jnp.concatenate([turned[:, count:], turned[:, :count]], axis=1)
        return jnp.where(bit == 1, turned, matrix)

    block(steer_ref, steering_ref[0], steering_ref[1])
    for level in range(merge_re_ref.shape[0]):
        bit = (member_ref[0] >> level) & 1
        block(
            merge_ref.at[level], arranged(merge_re_ref[level], bit), arranged(merge_im_ref[level], bit)
        )


def windows_kernel(own, halo, member_ref, raw_ref, *rest):
    outs, sems = rest[: SET + 2], rest[SET + 2]
    member = member_ref[0]
    main, edge = 2 * own, 2 * halo
    early = own + edge

    def each(action):
        for slot in range(SET):
            block = swapped(member ^ slot)
            start = block * main

            def move(kind, source, out, target, length):
                made = pltpu.make_async_copy(
                    raw_ref.at[pl.ds(pl.multiple_of(source, 16), length), :],
                    out.at[pl.ds(target, length), :],
                    sems.at[slot, kind],
                )
                action(made)

            out = outs[slot]
            if slot < SET - 2:
                last, place = out, edge + main
                move(0, start, out, edge, main)
            else:
                last, place = outs[slot + 2], main - early
                move(0, start, out, edge, early)
                move(3, start + early, last, 0, main - early)

            @pl.when(block > 0)
            def _():
                move(1, start - edge, out, 0, edge)

            @pl.when(block < SET - 1)
            def _():
                move(2, start + main, last, place, edge)

    each(lambda made: made.start())
    zeros = jnp.zeros((edge, raw_ref.shape[1]), raw_ref.dtype)
    for slot in range(SET):
        block = swapped(member ^ slot)
        last = outs[slot] if slot < SET - 2 else outs[slot + 2]

        @pl.when(block == 0)
        def _():
            outs[slot][:edge, :] = zeros

        @pl.when(block == SET - 1)
        def _():
            last[last.shape[0] - edge :, :] = zeros

    each(lambda made: made.wait())


def moved_rows(value, table):
    pick, before, after = table
    chunk = value.shape[0] - 2 * SHIFT
    value = value.astype(jnp.float32)
    turned = [
        jnp.take_along_axis(value[tile * SHIFT : (tile + 1) * SHIFT], pick, axis=0)
        for tile in range(chunk // SHIFT + 2)
    ]
    moved = [
        jnp.where(before, turned[tile], jnp.where(after, turned[tile + 2], turned[tile + 1]))
        for tile in range(chunk // SHIFT)
    ]
    return jnp.concatenate(moved, axis=0).astype(jnp.bfloat16)


def merge_level(rows, level, pairs, member, load, sources, merge, shift_ref, emit):
    count = shift_ref.shape[2]
    sublane = lax.broadcasted_iota(jnp.int32, (SHIFT, count), 0)
    bit = (member >> level) & 1
    lower, upper = shift_ref[level, 0:1, :], shift_ref[level, 1:2, :]
    tables = []
    for own, other in ((lower, upper), (upper, lower)):
        offset = jnp.broadcast_to(jnp.where(bit == 0, own, other), (SHIFT, count)) + sublane
        tables.append((offset & (SHIFT - 1), offset < 0, offset >= SHIFT))

    def fill(at):
        target = sources[at % 2]
        for side in range(2):
            for part in range(2):
                column = (2 * part + side) * count
                low = 0
                while low < rows:
                    chunk = min(112, rows - low)
                    value = load(pairs[at][side], part, slice(low, low + chunk + 2 * SHIFT))
                    target[low : low + chunk, column : column + count] = moved_rows(value, tables[side])
                    low += chunk

    fill(0)
    for at, ends in enumerate(pairs):
        if at + 1 < len(pairs):
            fill(at + 1)
        for part in range(2):
            result = jnp.dot(
                sources[at % 2][...],
                merge[:, 2 * part * count : 2 * (part + 1) * count],
                preferred_element_type=jnp.float32,
            ).astype(jnp.bfloat16)
            for side in range(2):
                emit(ends[side], part, result[:, side * count : (side + 1) * count])


def fill_guards(beams, slots, rows):
    zeros = jnp.zeros((SHIFT, beams.shape[-1]), beams.dtype)
    for slot in range(slots):
        for part in range(2):
            beams[slot, part, :SHIFT, :] = zeros
            beams[slot, part, SHIFT + rows :, :] = zeros


def clear_outside(halo, member, beams, slots, ends):
    zeros = jnp.zeros((halo, beams.shape[-1]), beams.dtype)
    for end in ends:
        at = SHIFT if end == 0 else beams.shape[2] - SHIFT - halo

        @pl.when(member == end)
        def _():
            for slot in range(slots):
                for part in range(2):
                    beams[slot, part, at : at + halo, :] = zeros


def start_kernel(rows, halo, known, ends, member_ref, *rest):
    many = 2 if known else 1
    sources_of, rest = (rest[:many], rest[many : 2 * many]), rest[2 * many :]
    steer_ref, merge_ref, shift_ref, out_ref, beams, *sources, spread = rest
    count = steer_ref.shape[1] // 2
    member = member_ref[0]
    fill_guards(beams, 2, rows)
    fill_guards(out_ref, 2, rows)
    for slot, raw_refs in enumerate(sources_of):
        if known:
            spread[:known, :] = raw_refs[0][raw_refs[0].shape[0] - known :, :].astype(jnp.float32)
        spread[known:, :] = raw_refs[-1][...].astype(jnp.float32)
        real = spread[pl.ds(0, rows, stride=2), :].astype(jnp.bfloat16)
        imag = spread[pl.ds(1, rows, stride=2), :].astype(jnp.bfloat16)
        result = jnp.dot(
            jnp.concatenate([real, imag], axis=1), steer_ref[...], preferred_element_type=jnp.float32
        ).astype(jnp.bfloat16)
        beams[slot, 0, pl.ds(SHIFT, rows), :] = result[:, :count]
        beams[slot, 1, pl.ds(SHIFT, rows), :] = result[:, count:]

    def emit(slot, part, value):
        out_ref[slot, part, pl.ds(SHIFT, rows), :] = value

    def load(slot, part, window):
        return beams[slot, part, window, :]

    merge_level(rows, 0, [(0, 1)], member, load, sources, merge_ref.at[0], shift_ref, emit)
    clear_outside(halo, member, out_ref, 2, ends)


def middle_kernel(rows, halo, member_ref, left_ref, right_ref, merge_ref, shift_ref, out_ref, *sources):
    member = member_ref[0]
    fill_guards(out_ref, SET // 2, rows)

    def load(slot, part, window):
        return (left_ref, right_ref)[slot // 2][slot % 2, part, window, :]

    def emit(slot, part, value):
        out_ref[slot, part, pl.ds(SHIFT, rows), :] = value

    merge_level(rows, 1, [(0, 2), (1, 3)], member, load, sources, merge_ref.at[1], shift_ref, emit)
    clear_outside(halo, member, out_ref, SET // 2, (0, SET - 1))


def finish_kernel(
    rows, halo, begin, end, member_ref, middle_ref, left_ref, right_ref, merge_ref, shift_ref, out_ref,
    high, *sources,
):
    member = member_ref[0]
    fill_guards(high, SET // 2, rows)

    def within(window):
        return slice(begin + window.start, begin + window.stop)

    def load_pairs(slot, part, window):
        if slot < 2:
            return left_ref[slot, part, within(window), :]
        return right_ref[slot - 2, part, window, :]

    def load_all(slot, part, window):
        if slot < SET // 2:
            return middle_ref[slot, part, within(window), :]
        return high[slot - SET // 2, part, window, :]

    def keep(slot, part, value):
        high[slot, part, pl.ds(SHIFT, rows), :] = value

    def last(slot, part, value):
        out_ref[slot, part] = value[halo : rows - halo]

    merge_level(
        rows, 1, [(0, 2), (1, 3)], member, load_pairs, sources, merge_ref.at[1], shift_ref, keep
    )
    clear_outside(halo, member, high, SET // 2, (end,))
    pairs = [(slot, slot + SET // 2) for slot in range(SET // 2)]
    merge_level(rows, 2, pairs, member, load_all, sources, merge_ref.at[2], shift_ref, last)


def image_kernel(groups, *rest):
    known_refs, (beams_ref, *rest) = rest[: len(rest) - SET - 4], rest[len(rest) - SET - 4 :]
    maps, halves, out_ref = rest[: SET - 2], rest[SET - 2 : SET + 2], rest[SET + 2]
    own = beams_ref.shape[2]
    width = maps[0].shape[1]
    piece = out_ref.shape[2]
    first = 0
    if known_refs:
        first = known_refs[0].shape[1]
        out_ref[:, :first] = known_refs[0][...]
    values = [ref[...] for ref in maps] + [
        jnp.concatenate([halves[at][...], halves[at + 1][...]], axis=0) for at in (0, 2)
    ]
    for half in range(2):
        total = jnp.zeros((own, width), jnp.float32)
        for slot in range(SET):
            real, imag = beams_ref[slot, 0], beams_ref[slot, 1]
            left = jnp.concatenate([real, -imag] if half == 0 else [imag, real], axis=1)
            total += jnp.dot(left, values[slot], preferred_element_type=jnp.float32)
        total = total.astype(jnp.bfloat16)
        for at in range(own // piece):
            out_ref[
                swapped(at % groups), first + at // groups, :, half * width : (half + 1) * width
            ] = total[at * piece : (at + 1) * piece]


def sum_kernel(pieces_ref, out_ref):
    total = pieces_ref[0].astype(jnp.float32)
    for source in range(1, pieces_ref.shape[0]):
        total += pieces_ref[source].astype(jnp.float32)
    total = total.astype(jnp.bfloat16)
    out_ref[0] = total
    out_ref[1] = total


def last_kernel(half_ref, pieces_ref, out_ref):
    many = pieces_ref.shape[0] // 2
    base = half_ref[0] * many
    total = pieces_ref[base].astype(jnp.float32)
    for source in range(1, many):
        total += pieces_ref[base + source].astype(jnp.float32)
    out_ref[...] = total


def call(kernel, out_shape, in_specs, scratch=(), flops=0, vmem=24, out_specs=None):
    def run(*operands):
        return called(kernel, out_shape, in_specs, scratch, flops, vmem, out_specs)(*operands)

    return run


def called(kernel, out_shape, in_specs, scratch, flops, vmem, out_specs):
    return pl.pallas_call(
        kernel,
        out_shape=out_shape,
        in_specs=in_specs,
        out_specs=jax.tree.map(lambda _: VMEM, out_shape) if out_specs is None else out_specs,
        scratch_shapes=scratch,
        cost_estimate=pl.CostEstimate(flops=flops, bytes_accessed=2**20, transcendentals=0),
        compiler_params=pltpu.CompilerParams(vmem_limit_bytes=vmem * 2**20),
    )


def body(pulses, steering, merge_re, merge_im, range_shift, image_map):
    total_rows = pulses.shape[0]
    count = steering.shape[2]
    levels = merge_re.shape[0]
    groups = lax.axis_size("pulse")
    tiles = lax.axis_size("tile")
    sets = tiles // SET
    own = total_rows // SET
    halo = levels * SHIFT
    rows = own + 2 * halo
    piece = own // tiles
    half_type = jnp.bfloat16
    member = lax.axis_index("tile") % SET
    where = member.reshape(1).astype(jnp.int32)

    def swap(value, mask):
        return lax.ppermute(value, "tile", [(s, s ^ mask) for s in range(tiles)])

    part = own // 2 + 2 * halo
    raw = pulses.reshape(2 * total_rows, count)
    lengths = [2 * rows] * (SET - 2) + [2 * part] * 2 + [own] * 2
    windows = call(
        functools.partial(windows_kernel, own, halo),
        [jax.ShapeDtypeStruct((length, count), half_type) for length in lengths],
        [SMEM, pl.BlockSpec(memory_space=pltpu.HBM)],
        scratch=[pltpu.SemaphoreType.DMA((SET, 4))],
    )(where, raw)
    arrived = {0: windows[0]}
    for mask in range(1, SET):
        arrived[mask] = swap(windows[mask], mask)
    late = [swap(windows[mask + 2], mask) for mask in (6, 7)]

    own_map = image_map.reshape(2 * count, -1)
    width = own_map.shape[1]
    held = {0: own_map}
    for mask in (2, 4):
        held[mask] = swap(own_map, mask)
    for slot in (0, 2, 4):
        held[slot | 1] = swap(held[slot], 1)
    far = (swap(held[4][:count], 2), swap(held[2][count:], 4))
    near = (swap(far[0], 1), swap(far[1], 1))

    steer_block, merge_block = call(
        weights_kernel,
        [
            jax.ShapeDtypeStruct((2 * count, 2 * count), half_type),
            jax.ShapeDtypeStruct((levels, 4 * count, 4 * count), half_type),
        ],
        [SMEM] + [VMEM] * 3,
        flops=10**8,
    )(where, steering, merge_re, merge_im)

    def start(length, known, ends, *windows):
        return call(
            functools.partial(start_kernel, length, halo, known, ends),
            jax.ShapeDtypeStruct((2, 2, length + 2 * SHIFT, count), half_type),
            [SMEM] + [VMEM] * (3 + len(windows)),
            scratch=[
                pltpu.VMEM((2, 2, length + 2 * SHIFT, count), half_type),
                pltpu.VMEM((length, 4 * count), half_type),
                pltpu.VMEM((2 * length, count), jnp.float32),
            ],
            flops=5 * 10**8,
        )(where, *windows, steer_block, merge_block, range_shift)

    started = [
        start(rows, 0, (0, SET - 1), arrived[base], arrived[base + 1])
        for base in range(0, SET - 2, 2)
    ]
    middle = call(
        functools.partial(middle_kernel, rows, halo),
        jax.ShapeDtypeStruct((SET // 2, 2, rows + 2 * SHIFT, count), half_type),
        [SMEM] + [VMEM] * 4,
        scratch=[pltpu.VMEM((rows, 4 * count), half_type)] * 2,
        flops=6 * 10**8,
    )(where, started[0], started[1], merge_block, range_shift)
    partial_rows = ()
    for step in range(2):
        if step == 0:
            ending = start(part, 0, (0,), arrived[6], arrived[7])
        else:
            ending = start(part, 4 * halo, (SET - 1,), arrived[6], late[0], arrived[7], late[1])
        beams = call(
            functools.partial(finish_kernel, part, halo, step * own // 2, step * (SET - 1)),
            jax.ShapeDtypeStruct((SET, 2, own // 2, count), half_type),
            [SMEM] + [VMEM] * 5,
            scratch=[pltpu.VMEM((SET // 2, 2, part + 2 * SHIFT, count), half_type)]
            + [pltpu.VMEM((part, 4 * count), half_type)] * 2,
            flops=10**9,
        )(where, middle, started[2], ending, merge_block, range_shift)
        partial_rows = (
            call(
                functools.partial(image_kernel, groups),
                jax.ShapeDtypeStruct((groups, (1 + step) * sets // 2, piece, 2 * width), half_type),
                [VMEM] * (3 + SET + step),
                flops=10**9,
            )(*partial_rows, beams, *[held[slot] for slot in range(SET - 2)], *far, *near),
        )
    partial_rows = partial_rows[0]

    pieces = lax.all_to_all(partial_rows, "pulse", 0, 0, tiled=True)
    doubled = call(
        sum_kernel, jax.ShapeDtypeStruct((2, sets, piece, 2 * width), half_type), [VMEM]
    )(pieces)

    def device(pulse, u, i):
        return pulse * tiles + u * SET + swapped(i)

    crossing = []
    for a in range(groups):
        for b in range(a + 1, groups):
            crossing.append(
                [device(a, u, b) for u in range(sets)] + [device(b, u, a) for u in range(sets)]
            )
    for a in range(0, groups, 2):
        crossing.append(
            [device(a, u, a) for u in range(sets)] + [device(a + 1, u, a + 1) for u in range(sets)]
        )
    last = lax.all_to_all(
        doubled.reshape(2 * sets, piece, 2 * width),
        ("pulse", "tile"),
        0,
        0,
        axis_index_groups=crossing,
        tiled=True,
    )
    pulse = lax.axis_index("pulse")
    target = swapped(member)
    half = jnp.where(pulse == target, pulse % 2, (pulse < target).astype(jnp.int32))
    return call(
        last_kernel, jax.ShapeDtypeStruct((piece, 2 * width), jnp.float32), [SMEM, VMEM]
    )(half.reshape(1).astype(jnp.int32), last)


def solution(mesh):
    placed = (
        P(None, None, ("pulse", "tile")),
        P(),
        P(),
        P(),
        P(),
        P("pulse", "tile", None, None, None),
    )
    return jax.shard_map(
        body, mesh=mesh, in_specs=placed, out_specs=P(("pulse", "tile"), None), check_vma=False
    )
```

```python
import functools

import jax
import jax.numpy as jnp
from jax import lax
from jax.experimental import pallas as pl
from jax.experimental.pallas import tpu as pltpu
from jax.sharding import PartitionSpec as P


SHIFT = 8
SET = 8
VMEM = pl.BlockSpec(memory_space=pltpu.VMEM)
SMEM = pl.BlockSpec(memory_space=pltpu.SMEM)


def swapped(index):
    return ((index >> 1) & 1) << 2 | ((index >> 2) & 1) << 1 | (index & 1)


def weights_kernel(member_ref, steering_ref, merge_re_ref, merge_im_ref, steer_ref, merge_ref):
    def block(out, real, imag):
        high, wide = real.shape
        out[:high, :wide] = real
        out[:high, wide:] = imag
        out[high:, :wide] = -imag
        out[high:, wide:] = real

    def arranged(matrix, bit):
        count = matrix.shape[0] // 2
        turned = jnp.concatenate([matrix[count:], matrix[:count]], axis=0)
        turned = jnp.concatenate([turned[:, count:], turned[:, :count]], axis=1)
        return jnp.where(bit == 1, turned, matrix)

    block(steer_ref, steering_ref[0], steering_ref[1])
    for level in range(merge_re_ref.shape[0]):
        bit = ((member_ref[0] & (SET - 1)) >> level) & 1
        block(
            merge_ref.at[level], arranged(merge_re_ref[level], bit), arranged(merge_im_ref[level], bit)
        )


def windows_kernel(own, halo, member_ref, raw_ref, *rest):
    outs, sems = rest[: SET + 2], rest[SET + 2]
    member = (member_ref[0] & (SET - 1))
    main, edge = 2 * own, 2 * halo
    early = own + edge

    def each(action):
        for slot in range(SET):
            block = swapped(member ^ slot)
            start = block * main

            def move(kind, source, out, target, length):
                made = pltpu.make_async_copy(
                    raw_ref.at[pl.ds(pl.multiple_of(source, 16), length), :],
                    out.at[pl.ds(target, length), :],
                    sems.at[slot, kind],
                )
                action(made)

            out = outs[slot]
            if slot < SET - 2:
                last, place = out, edge + main
                move(0, start, out, edge, main)
            else:
                last, place = outs[slot + 2], main - early
                move(0, start, out, edge, early)
                move(3, start + early, last, 0, main - early)

            @pl.when(block > 0)
            def _():
                move(1, start - edge, out, 0, edge)

            @pl.when(block < SET - 1)
            def _():
                move(2, start + main, last, place, edge)

    each(lambda made: made.start())
    zeros = jnp.zeros((edge, raw_ref.shape[1]), raw_ref.dtype)
    for slot in range(SET):
        block = swapped(member ^ slot)
        last = outs[slot] if slot < SET - 2 else outs[slot + 2]

        @pl.when(block == 0)
        def _():
            outs[slot][:edge, :] = zeros

        @pl.when(block == SET - 1)
        def _():
            last[last.shape[0] - edge :, :] = zeros

    each(lambda made: made.wait())


def moved_rows(value, table):
    pick, before, after = table
    chunk = value.shape[0] - 2 * SHIFT
    value = value.astype(jnp.float32)
    turned = [
        jnp.take_along_axis(value[tile * SHIFT : (tile + 1) * SHIFT], pick, axis=0)
        for tile in range(chunk // SHIFT + 2)
    ]
    moved = [
        jnp.where(before, turned[tile], jnp.where(after, turned[tile + 2], turned[tile + 1]))
        for tile in range(chunk // SHIFT)
    ]
    return jnp.concatenate(moved, axis=0).astype(jnp.bfloat16)


def merge_level(rows, level, pairs, member, load, sources, merge, shift_ref, emit):
    count = shift_ref.shape[2]
    sublane = lax.broadcasted_iota(jnp.int32, (SHIFT, count), 0)
    bit = (member >> level) & 1
    lower, upper = shift_ref[level, 0:1, :], shift_ref[level, 1:2, :]
    tables = []
    for own, other in ((lower, upper), (upper, lower)):
        offset = jnp.broadcast_to(jnp.where(bit == 0, own, other), (SHIFT, count)) + sublane
        tables.append((offset & (SHIFT - 1), offset < 0, offset >= SHIFT))

    def fill(at):
        target = sources[at % 2]
        for side in range(2):
            for part in range(2):
                column = (2 * part + side) * count
                low = 0
                while low < rows:
                    chunk = min(112, rows - low)
                    value = load(pairs[at][side], part, slice(low, low + chunk + 2 * SHIFT))
                    target[low : low + chunk, column : column + count] = moved_rows(value, tables[side])
                    low += chunk

    fill(0)
    for at, ends in enumerate(pairs):
        if at + 1 < len(pairs):
            fill(at + 1)
        for part in range(2):
            result = jnp.dot(
                sources[at % 2][...],
                merge[:, 2 * part * count : 2 * (part + 1) * count],
                preferred_element_type=jnp.float32,
            ).astype(jnp.bfloat16)
            for side in range(2):
                emit(ends[side], part, result[:, side * count : (side + 1) * count])


def fill_guards(beams, slots, rows):
    zeros = jnp.zeros((SHIFT, beams.shape[-1]), beams.dtype)
    for slot in range(slots):
        for part in range(2):
            beams[slot, part, :SHIFT, :] = zeros
            beams[slot, part, SHIFT + rows :, :] = zeros


def clear_outside(halo, member, beams, slots, ends):
    zeros = jnp.zeros((halo, beams.shape[-1]), beams.dtype)
    for end in ends:
        at = SHIFT if end == 0 else beams.shape[2] - SHIFT - halo

        @pl.when(member == end)
        def _():
            for slot in range(slots):
                for part in range(2):
                    beams[slot, part, at : at + halo, :] = zeros


def start_kernel(rows, halo, known, ends, member_ref, *rest):
    many = 2 if known else 1
    sources_of, rest = (rest[:many], rest[many : 2 * many]), rest[2 * many :]
    steer_ref, merge_ref, shift_ref, out_ref, beams, *sources, spread = rest
    count = steer_ref.shape[1] // 2
    member = (member_ref[0] & (SET - 1))
    fill_guards(beams, 2, rows)
    fill_guards(out_ref, 2, rows)
    for slot, raw_refs in enumerate(sources_of):
        if known:
            spread[:known, :] = raw_refs[0][raw_refs[0].shape[0] - known :, :].astype(jnp.float32)
        spread[known:, :] = raw_refs[-1][...].astype(jnp.float32)
        real = spread[pl.ds(0, rows, stride=2), :].astype(jnp.bfloat16)
        imag = spread[pl.ds(1, rows, stride=2), :].astype(jnp.bfloat16)
        result = jnp.dot(
            jnp.concatenate([real, imag], axis=1), steer_ref[...], preferred_element_type=jnp.float32
        ).astype(jnp.bfloat16)
        beams[slot, 0, pl.ds(SHIFT, rows), :] = result[:, :count]
        beams[slot, 1, pl.ds(SHIFT, rows), :] = result[:, count:]

    def emit(slot, part, value):
        out_ref[slot, part, pl.ds(SHIFT, rows), :] = value

    def load(slot, part, window):
        return beams[slot, part, window, :]

    merge_level(rows, 0, [(0, 1)], member, load, sources, merge_ref.at[0], shift_ref, emit)
    clear_outside(halo, member, out_ref, 2, ends)


def middle_kernel(rows, halo, member_ref, left_ref, right_ref, merge_ref, shift_ref, out_ref, *sources):
    member = (member_ref[0] & (SET - 1))
    fill_guards(out_ref, SET // 2, rows)

    def load(slot, part, window):
        return (left_ref, right_ref)[slot // 2][slot % 2, part, window, :]

    def emit(slot, part, value):
        out_ref[slot, part, pl.ds(SHIFT, rows), :] = value

    merge_level(rows, 1, [(0, 2), (1, 3)], member, load, sources, merge_ref.at[1], shift_ref, emit)
    clear_outside(halo, member, out_ref, SET // 2, (0, SET - 1))


def finish_kernel(
    rows, halo, begin, end, member_ref, middle_ref, left_ref, right_ref, merge_ref, shift_ref, out_ref,
    high, *sources,
):
    member = (member_ref[0] & (SET - 1))
    fill_guards(high, SET // 2, rows)

    def within(window):
        return slice(begin + window.start, begin + window.stop)

    def load_pairs(slot, part, window):
        if slot < 2:
            return left_ref[slot, part, within(window), :]
        return right_ref[slot - 2, part, window, :]

    def load_all(slot, part, window):
        if slot < SET // 2:
            return middle_ref[slot, part, within(window), :]
        return high[slot - SET // 2, part, window, :]

    def keep(slot, part, value):
        high[slot, part, pl.ds(SHIFT, rows), :] = value

    def last(slot, part, value):
        out_ref[slot, part] = value[halo : rows - halo]

    merge_level(
        rows, 1, [(0, 2), (1, 3)], member, load_pairs, sources, merge_ref.at[1], shift_ref, keep
    )
    clear_outside(halo, member, high, SET // 2, (end,))
    pairs = [(slot, slot + SET // 2) for slot in range(SET // 2)]
    merge_level(rows, 2, pairs, member, load_all, sources, merge_ref.at[2], shift_ref, last)


def image_kernel(groups, *rest):
    known_refs, (beams_ref, *rest) = rest[: len(rest) - SET - 4], rest[len(rest) - SET - 4 :]
    maps, halves, out_ref = rest[: SET - 2], rest[SET - 2 : SET + 2], rest[SET + 2]
    own = beams_ref.shape[2]
    width = maps[0].shape[1]
    piece = out_ref.shape[2]
    first = 0
    if known_refs:
        first = known_refs[0].shape[1]
        out_ref[:, :first] = known_refs[0][...]
    values = [ref[...] for ref in maps] + [
        jnp.concatenate([halves[at][...], halves[at + 1][...]], axis=0) for at in (0, 2)
    ]
    for half in range(2):
        total = jnp.zeros((own, width), jnp.float32)
        for slot in range(SET):
            real, imag = beams_ref[slot, 0], beams_ref[slot, 1]
            left = jnp.concatenate([real, -imag] if half == 0 else [imag, real], axis=1)
            total += jnp.dot(left, values[slot], preferred_element_type=jnp.float32)
        total = total.astype(jnp.bfloat16)
        for at in range(own // piece):
            out_ref[
                swapped(at % groups), first + at // groups, :, half * width : (half + 1) * width
            ] = total[at * piece : (at + 1) * piece]


def sum_kernel(pieces_ref, out_ref):
    many = pieces_ref.shape[1]
    for at in range(many):
        total = pieces_ref[0, at].astype(jnp.float32)
        for source in range(1, pieces_ref.shape[0]):
            total += pieces_ref[source, at].astype(jnp.float32)
        total = total.astype(jnp.bfloat16)
        out_ref[0, at] = total
        out_ref[1, at] = total


def last_kernel(half_ref, pieces_ref, out_ref):
    many = pieces_ref.shape[0] // 2
    base = (half_ref[0] >> 3) * many
    total = pieces_ref[base].astype(jnp.float32)
    for source in range(1, many):
        total += pieces_ref[base + source].astype(jnp.float32)
    out_ref[...] = total


def call(kernel, out_shape, in_specs, scratch=(), flops=0, vmem=24, out_specs=None):
    def run(*operands):
        return called(kernel, out_shape, in_specs, scratch, flops, vmem, out_specs)(*operands)

    return run


def called(kernel, out_shape, in_specs, scratch, flops, vmem, out_specs):
    return pl.pallas_call(
        kernel,
        out_shape=out_shape,
        in_specs=in_specs,
        out_specs=jax.tree.map(lambda _: VMEM, out_shape) if out_specs is None else out_specs,
        scratch_shapes=scratch,
        cost_estimate=pl.CostEstimate(flops=flops, bytes_accessed=2**20, transcendentals=0),
        compiler_params=pltpu.CompilerParams(vmem_limit_bytes=vmem * 2**20),
    )


def body(pulses, steering, merge_re, merge_im, range_shift, image_map):
    total_rows = pulses.shape[0]
    count = steering.shape[2]
    levels = merge_re.shape[0]
    groups = lax.axis_size("pulse")
    tiles = lax.axis_size("tile")
    sets = tiles // SET
    own = total_rows // SET
    halo = levels * SHIFT
    rows = own + 2 * halo
    piece = own // tiles
    half_type = jnp.bfloat16
    member = lax.axis_index("tile") % SET
    pulse = lax.axis_index("pulse")
    target = swapped(member)
    half = jnp.where(pulse == target, pulse % 2, (pulse < target).astype(jnp.int32))
    where = (member + SET * half).reshape(1).astype(jnp.int32)

    def swap(value, mask):
        return lax.ppermute(value, "tile", [(s, s ^ mask) for s in range(tiles)])

    part = own // 2 + 2 * halo
    raw = pulses.reshape(2 * total_rows, count)
    lengths = [2 * rows] * (SET - 2) + [2 * part] * 2 + [own] * 2
    windows = call(
        functools.partial(windows_kernel, own, halo),
        [jax.ShapeDtypeStruct((length, count), half_type) for length in lengths],
        [SMEM, pl.BlockSpec(memory_space=pltpu.HBM)],
        scratch=[pltpu.SemaphoreType.DMA((SET, 4))],
    )(where, raw)
    arrived = {0: windows[0]}
    for mask in range(1, SET):
        arrived[mask] = swap(windows[mask], mask)
    late = [swap(windows[mask + 2], mask) for mask in (6, 7)]

    own_map = image_map.reshape(2 * count, -1)
    width = own_map.shape[1]
    held = {0: own_map}
    for mask in (2, 4):
        held[mask] = swap(own_map, mask)
    for slot in (0, 2, 4):
        held[slot | 1] = swap(held[slot], 1)
    far = (swap(held[4][:count], 2), swap(held[2][count:], 4))
    near = (swap(far[0], 1), swap(far[1], 1))

    steer_block, merge_block = call(
        weights_kernel,
        [
            jax.ShapeDtypeStruct((2 * count, 2 * count), half_type),
            jax.ShapeDtypeStruct((levels, 4 * count, 4 * count), half_type),
        ],
        [SMEM] + [VMEM] * 3,
        flops=10**8,
    )(where, steering, merge_re, merge_im)

    def start(length, known, ends, *windows):
        return call(
            functools.partial(start_kernel, length, halo, known, ends),
            jax.ShapeDtypeStruct((2, 2, length + 2 * SHIFT, count), half_type),
            [SMEM] + [VMEM] * (3 + len(windows)),
            scratch=[
                pltpu.VMEM((2, 2, length + 2 * SHIFT, count), half_type),
                pltpu.VMEM((length, 4 * count), half_type),
                pltpu.VMEM((2 * length, count), jnp.float32),
            ],
            flops=5 * 10**8,
        )(where, *windows, steer_block, merge_block, range_shift)

    started = [
        start(rows, 0, (0, SET - 1), arrived[base], arrived[base + 1])
        for base in range(0, SET - 2, 2)
    ]
    middle = call(
        functools.partial(middle_kernel, rows, halo),
        jax.ShapeDtypeStruct((SET // 2, 2, rows + 2 * SHIFT, count), half_type),
        [SMEM] + [VMEM] * 4,
        scratch=[pltpu.VMEM((rows, 4 * count), half_type)] * 2,
        flops=6 * 10**8,
    )(where, started[0], started[1], merge_block, range_shift)
    partial_rows = ()
    for step in range(2):
        if step == 0:
            ending = start(part, 0, (0,), arrived[6], arrived[7])
        else:
            ending = start(part, 4 * halo, (SET - 1,), arrived[6], late[0], arrived[7], late[1])
        beams = call(
            functools.partial(finish_kernel, part, halo, step * own // 2, step * (SET - 1)),
            jax.ShapeDtypeStruct((SET, 2, own // 2, count), half_type),
            [SMEM] + [VMEM] * 5,
            scratch=[pltpu.VMEM((SET // 2, 2, part + 2 * SHIFT, count), half_type)]
            + [pltpu.VMEM((part, 4 * count), half_type)] * 2,
            flops=10**9,
        )(where, middle, started[2], ending, merge_block, range_shift)
        partial_rows = (
            call(
                functools.partial(image_kernel, groups),
                jax.ShapeDtypeStruct((groups, (1 + step) * sets // 2, piece, 2 * width), half_type),
                [VMEM] * (3 + SET + step),
                flops=10**9,
            )(*partial_rows, beams, *[held[slot] for slot in range(SET - 2)], *far, *near),
        )
    partial_rows = partial_rows[0]

    pieces = lax.all_to_all(partial_rows, "pulse", 0, 0, tiled=True)
    doubled = call(
        sum_kernel, jax.ShapeDtypeStruct((2, sets, piece, 2 * width), half_type), [VMEM]
    )(pieces)

    def device(pulse, u, i):
        return pulse * tiles + u * SET + swapped(i)

    crossing = []
    for a in range(groups):
        for b in range(a + 1, groups):
            crossing.append(
                [device(a, u, b) for u in range(sets)] + [device(b, u, a) for u in range(sets)]
            )
    for a in range(0, groups, 2):
        crossing.append(
            [device(a, u, a) for u in range(sets)] + [device(a + 1, u, a + 1) for u in range(sets)]
        )
    last = lax.all_to_all(
        doubled.reshape(2 * sets, piece, 2 * width),
        ("pulse", "tile"),
        0,
        0,
        axis_index_groups=crossing,
        tiled=True,
    )
    return call(
        last_kernel, jax.ShapeDtypeStruct((piece, 2 * width), jnp.float32), [SMEM, VMEM]
    )(where, last)


def solution(mesh):
    placed = (
        P(None, None, ("pulse", "tile")),
        P(),
        P(),
        P(),
        P(),
        P("pulse", "tile", None, None, None),
    )
    return jax.shard_map(
        body, mesh=mesh, in_specs=placed, out_specs=P(("pulse", "tile"), None), check_vma=False
    )
```

```python
import functools

import jax
import jax.numpy as jnp
from jax import lax
from jax.experimental import pallas as pl
from jax.experimental.pallas import tpu as pltpu
from jax.sharding import PartitionSpec as P


SHIFT = 8
SET = 8
VMEM = pl.BlockSpec(memory_space=pltpu.VMEM)
SMEM = pl.BlockSpec(memory_space=pltpu.SMEM)


def swapped(index):
    return ((index >> 1) & 1) << 2 | ((index >> 2) & 1) << 1 | (index & 1)


def weights_kernel(member_ref, steering_ref, merge_re_ref, merge_im_ref, steer_ref, merge_ref):
    def block(out, real, imag):
        high, wide = real.shape
        out[:high, :wide] = real
        out[:high, wide:] = imag
        out[high:, :wide] = -imag
        out[high:, wide:] = real

    def arranged(matrix, bit):
        count = matrix.shape[0] // 2
        turned = jnp.concatenate([matrix[count:], matrix[:count]], axis=0)
        turned = jnp.concatenate([turned[:, count:], turned[:, :count]], axis=1)
        return jnp.where(bit == 1, turned, matrix)

    block(steer_ref, steering_ref[0], steering_ref[1])
    for level in range(merge_re_ref.shape[0]):
        bit = ((member_ref[0] & (SET - 1)) >> level) & 1
        block(
            merge_ref.at[level], arranged(merge_re_ref[level], bit), arranged(merge_im_ref[level], bit)
        )


def windows_kernel(own, halo, member_ref, raw_ref, *rest):
    outs, sems = rest[: SET + 2], rest[SET + 2]
    member = (member_ref[0] & (SET - 1))
    main, edge = 2 * own, 2 * halo
    early = own + edge

    def each(action):
        for slot in range(SET):
            block = swapped(member ^ slot)
            start = block * main

            def move(kind, source, out, target, length):
                made = pltpu.make_async_copy(
                    raw_ref.at[pl.ds(pl.multiple_of(source, 16), length), :],
                    out.at[pl.ds(target, length), :],
                    sems.at[slot, kind],
                )
                action(made)

            out = outs[slot]
            if slot < SET - 2:
                last, place = out, edge + main
                move(0, start, out, edge, main)
            else:
                last, place = outs[slot + 2], main - early
                move(0, start, out, edge, early)
                move(3, start + early, last, 0, main - early)

            @pl.when(block > 0)
            def _():
                move(1, start - edge, out, 0, edge)

            @pl.when(block < SET - 1)
            def _():
                move(2, start + main, last, place, edge)

    each(lambda made: made.start())
    zeros = jnp.zeros((edge, raw_ref.shape[1]), raw_ref.dtype)
    for slot in range(SET):
        block = swapped(member ^ slot)
        last = outs[slot] if slot < SET - 2 else outs[slot + 2]

        @pl.when(block == 0)
        def _():
            outs[slot][:edge, :] = zeros

        @pl.when(block == SET - 1)
        def _():
            last[last.shape[0] - edge :, :] = zeros

    each(lambda made: made.wait())


def moved_rows(value, table):
    pick, before, after = table
    chunk = value.shape[0] - 2 * SHIFT
    value = value.astype(jnp.float32)
    turned = [
        jnp.take_along_axis(value[tile * SHIFT : (tile + 1) * SHIFT], pick, axis=0)
        for tile in range(chunk // SHIFT + 2)
    ]
    moved = [
        jnp.where(before, turned[tile], jnp.where(after, turned[tile + 2], turned[tile + 1]))
        for tile in range(chunk // SHIFT)
    ]
    return jnp.concatenate(moved, axis=0).astype(jnp.bfloat16)


def merge_level(rows, level, pairs, member, load, sources, merge, shift_ref, emit):
    count = shift_ref.shape[2]
    sublane = lax.broadcasted_iota(jnp.int32, (SHIFT, count), 0)
    bit = (member >> level) & 1
    lower, upper = shift_ref[level, 0:1, :], shift_ref[level, 1:2, :]
    tables = []
    for own, other in ((lower, upper), (upper, lower)):
        offset = jnp.broadcast_to(jnp.where(bit == 0, own, other), (SHIFT, count)) + sublane
        tables.append((offset & (SHIFT - 1), offset < 0, offset >= SHIFT))

    def fill(at):
        target = sources[at % 2]
        for side in range(2):
            for part in range(2):
                column = (2 * part + side) * count
                low = 0
                while low < rows:
                    chunk = min(112, rows - low)
                    value = load(pairs[at][side], part, slice(low, low + chunk + 2 * SHIFT))
                    target[low : low + chunk, column : column + count] = moved_rows(value, tables[side])
                    low += chunk

    fill(0)
    for at, ends in enumerate(pairs):
        if at + 1 < len(pairs):
            fill(at + 1)
        for part in range(2):
            result = jnp.dot(
                sources[at % 2][...],
                merge[:, 2 * part * count : 2 * (part + 1) * count],
                preferred_element_type=jnp.float32,
            ).astype(jnp.bfloat16)
            for side in range(2):
                emit(ends[side], part, result[:, side * count : (side + 1) * count])


def fill_guards(beams, slots, rows):
    zeros = jnp.zeros((SHIFT, beams.shape[-1]), beams.dtype)
    for slot in range(slots):
        for part in range(2):
            beams[slot, part, :SHIFT, :] = zeros
            beams[slot, part, SHIFT + rows :, :] = zeros


def clear_outside(halo, member, beams, slots, ends):
    zeros = jnp.zeros((halo, beams.shape[-1]), beams.dtype)
    for end in ends:
        at = SHIFT if end == 0 else beams.shape[2] - SHIFT - halo

        @pl.when(member == end)
        def _():
            for slot in range(slots):
                for part in range(2):
                    beams[slot, part, at : at + halo, :] = zeros


def start_kernel(rows, halo, known, ends, member_ref, *rest):
    many = 2 if known else 1
    sources_of, rest = (rest[:many], rest[many : 2 * many]), rest[2 * many :]
    steer_ref, merge_ref, shift_ref, out_ref, beams, *sources, spread = rest
    count = steer_ref.shape[1] // 2
    member = (member_ref[0] & (SET - 1))
    fill_guards(beams, 2, rows)
    fill_guards(out_ref, 2, rows)
    for slot, raw_refs in enumerate(sources_of):
        if known:
            spread[:known, :] = raw_refs[0][raw_refs[0].shape[0] - known :, :].astype(jnp.float32)
        spread[known:, :] = raw_refs[-1][...].astype(jnp.float32)
        real = spread[pl.ds(0, rows, stride=2), :].astype(jnp.bfloat16)
        imag = spread[pl.ds(1, rows, stride=2), :].astype(jnp.bfloat16)
        result = jnp.dot(
            jnp.concatenate([real, imag], axis=1), steer_ref[...], preferred_element_type=jnp.float32
        ).astype(jnp.bfloat16)
        beams[slot, 0, pl.ds(SHIFT, rows), :] = result[:, :count]
        beams[slot, 1, pl.ds(SHIFT, rows), :] = result[:, count:]

    def emit(slot, part, value):
        out_ref[slot, part, pl.ds(SHIFT, rows), :] = value

    def load(slot, part, window):
        return beams[slot, part, window, :]

    merge_level(rows, 0, [(0, 1)], member, load, sources, merge_ref.at[0], shift_ref, emit)
    clear_outside(halo, member, out_ref, 2, ends)


def middle_kernel(rows, halo, member_ref, left_ref, right_ref, merge_ref, shift_ref, out_ref, *sources):
    member = (member_ref[0] & (SET - 1))
    fill_guards(out_ref, SET // 2, rows)

    def load(slot, part, window):
        return (left_ref, right_ref)[slot // 2][slot % 2, part, window, :]

    def emit(slot, part, value):
        out_ref[slot, part, pl.ds(SHIFT, rows), :] = value

    merge_level(rows, 1, [(0, 2), (1, 3)], member, load, sources, merge_ref.at[1], shift_ref, emit)
    clear_outside(halo, member, out_ref, SET // 2, (0, SET - 1))


def finish_kernel(
    rows, halo, begin, end, member_ref, middle_ref, left_ref, right_ref, merge_ref, shift_ref, out_ref,
    high, *sources,
):
    member = (member_ref[0] & (SET - 1))
    fill_guards(high, SET // 2, rows)

    def within(window):
        return slice(begin + window.start, begin + window.stop)

    def load_pairs(slot, part, window):
        if slot < 2:
            return left_ref[slot, part, within(window), :]
        return right_ref[slot - 2, part, window, :]

    def load_all(slot, part, window):
        if slot < SET // 2:
            return middle_ref[slot, part, within(window), :]
        return high[slot - SET // 2, part, window, :]

    def keep(slot, part, value):
        high[slot, part, pl.ds(SHIFT, rows), :] = value

    def last(slot, part, value):
        out_ref[slot, part] = value[halo : rows - halo]

    merge_level(
        rows, 1, [(0, 2), (1, 3)], member, load_pairs, sources, merge_ref.at[1], shift_ref, keep
    )
    clear_outside(halo, member, high, SET // 2, (end,))
    pairs = [(slot, slot + SET // 2) for slot in range(SET // 2)]
    merge_level(rows, 2, pairs, member, load_all, sources, merge_ref.at[2], shift_ref, last)


def image_kernel(groups, *rest):
    known_refs, (beams_ref, *rest) = rest[: len(rest) - SET - 4], rest[len(rest) - SET - 4 :]
    maps, halves, out_ref = rest[: SET - 2], rest[SET - 2 : SET + 2], rest[SET + 2]
    own = beams_ref.shape[2]
    width = maps[0].shape[1]
    piece = out_ref.shape[2]
    first = 0
    if known_refs:
        first = known_refs[0].shape[1]
        out_ref[:, :first] = known_refs[0][...]
    values = [ref[...] for ref in maps] + [
        jnp.concatenate([halves[at][...], halves[at + 1][...]], axis=0) for at in (0, 2)
    ]
    for half in range(2):
        total = jnp.zeros((own, width), jnp.float32)
        for slot in range(SET):
            real, imag = beams_ref[slot, 0], beams_ref[slot, 1]
            left = jnp.concatenate([real, -imag] if half == 0 else [imag, real], axis=1)
            total += jnp.dot(left, values[slot], preferred_element_type=jnp.float32)
        total = total.astype(jnp.bfloat16)
        for at in range(own // piece):
            out_ref[
                swapped(at % groups), first + at // groups, :, half * width : (half + 1) * width
            ] = total[at * piece : (at + 1) * piece]


def sum_kernel(pieces_ref, out_ref):
    many = pieces_ref.shape[1]
    for at in range(many):
        total = pieces_ref[0, at].astype(jnp.float32)
        for source in range(1, pieces_ref.shape[0]):
            total += pieces_ref[source, at].astype(jnp.float32)
        total = total.astype(jnp.bfloat16)
        out_ref[at, 0] = total
        out_ref[at, 1] = total


def last_kernel(half_ref, pieces_ref, out_ref):
    many = pieces_ref.shape[0] // 2
    half = half_ref[0] >> 3
    total = pieces_ref[half].astype(jnp.float32)
    for source in range(1, many):
        total += pieces_ref[2 * source + half].astype(jnp.float32)
    out_ref[...] = total


def call(kernel, out_shape, in_specs, scratch=(), flops=0, vmem=24, out_specs=None):
    def run(*operands):
        return called(kernel, out_shape, in_specs, scratch, flops, vmem, out_specs)(*operands)

    return run


def called(kernel, out_shape, in_specs, scratch, flops, vmem, out_specs):
    return pl.pallas_call(
        kernel,
        out_shape=out_shape,
        in_specs=in_specs,
        out_specs=jax.tree.map(lambda _: VMEM, out_shape) if out_specs is None else out_specs,
        scratch_shapes=scratch,
        cost_estimate=pl.CostEstimate(flops=flops, bytes_accessed=2**20, transcendentals=0),
        compiler_params=pltpu.CompilerParams(vmem_limit_bytes=vmem * 2**20),
    )


def body(pulses, steering, merge_re, merge_im, range_shift, image_map):
    total_rows = pulses.shape[0]
    count = steering.shape[2]
    levels = merge_re.shape[0]
    groups = lax.axis_size("pulse")
    tiles = lax.axis_size("tile")
    sets = tiles // SET
    own = total_rows // SET
    halo = levels * SHIFT
    rows = own + 2 * halo
    piece = own // tiles
    half_type = jnp.bfloat16
    member = lax.axis_index("tile") % SET
    pulse = lax.axis_index("pulse")
    target = swapped(member)
    half = jnp.where(pulse == target, pulse % 2, (pulse < target).astype(jnp.int32))
    where = (member + SET * half).reshape(1).astype(jnp.int32)

    def swap(value, mask):
        return lax.ppermute(value, "tile", [(s, s ^ mask) for s in range(tiles)])

    part = own // 2 + 2 * halo
    raw = pulses.reshape(2 * total_rows, count)
    lengths = [2 * rows] * (SET - 2) + [2 * part] * 2 + [own] * 2
    windows = call(
        functools.partial(windows_kernel, own, halo),
        [jax.ShapeDtypeStruct((length, count), half_type) for length in lengths],
        [SMEM, pl.BlockSpec(memory_space=pltpu.HBM)],
        scratch=[pltpu.SemaphoreType.DMA((SET, 4))],
    )(where, raw)
    arrived = {0: windows[0]}
    for mask in range(1, SET):
        arrived[mask] = swap(windows[mask], mask)
    late = [swap(windows[mask + 2], mask) for mask in (6, 7)]

    own_map = image_map.reshape(2 * count, -1)
    width = own_map.shape[1]
    held = {0: own_map}
    for mask in (2, 4):
        held[mask] = swap(own_map, mask)
    for slot in (0, 2, 4):
        held[slot | 1] = swap(held[slot], 1)
    far = (swap(held[4][:count], 2), swap(held[2][count:], 4))
    near = (swap(far[0], 1), swap(far[1], 1))

    steer_block, merge_block = call(
        weights_kernel,
        [
            jax.ShapeDtypeStruct((2 * count, 2 * count), half_type),
            jax.ShapeDtypeStruct((levels, 4 * count, 4 * count), half_type),
        ],
        [SMEM] + [VMEM] * 3,
        flops=10**8,
    )(where, steering, merge_re, merge_im)

    def start(length, known, ends, *windows):
        return call(
            functools.partial(start_kernel, length, halo, known, ends),
            jax.ShapeDtypeStruct((2, 2, length + 2 * SHIFT, count), half_type),
            [SMEM] + [VMEM] * (3 + len(windows)),
            scratch=[
                pltpu.VMEM((2, 2, length + 2 * SHIFT, count), half_type),
                pltpu.VMEM((length, 4 * count), half_type),
                pltpu.VMEM((2 * length, count), jnp.float32),
            ],
            flops=5 * 10**8,
        )(where, *windows, steer_block, merge_block, range_shift)

    started = [
        start(rows, 0, (0, SET - 1), arrived[base], arrived[base + 1])
        for base in range(0, SET - 2, 2)
    ]
    middle = call(
        functools.partial(middle_kernel, rows, halo),
        jax.ShapeDtypeStruct((SET // 2, 2, rows + 2 * SHIFT, count), half_type),
        [SMEM] + [VMEM] * 4,
        scratch=[pltpu.VMEM((rows, 4 * count), half_type)] * 2,
        flops=6 * 10**8,
    )(where, started[0], started[1], merge_block, range_shift)
    partial_rows = ()
    for step in range(2):
        if step == 0:
            ending = start(part, 0, (0,), arrived[6], arrived[7])
        else:
            ending = start(part, 4 * halo, (SET - 1,), arrived[6], late[0], arrived[7], late[1])
        beams = call(
            functools.partial(finish_kernel, part, halo, step * own // 2, step * (SET - 1)),
            jax.ShapeDtypeStruct((SET, 2, own // 2, count), half_type),
            [SMEM] + [VMEM] * 5,
            scratch=[pltpu.VMEM((SET // 2, 2, part + 2 * SHIFT, count), half_type)]
            + [pltpu.VMEM((part, 4 * count), half_type)] * 2,
            flops=10**9,
        )(where, middle, started[2], ending, merge_block, range_shift)
        partial_rows = (
            call(
                functools.partial(image_kernel, groups),
                jax.ShapeDtypeStruct((groups, (1 + step) * sets // 2, piece, 2 * width), half_type),
                [VMEM] * (3 + SET + step),
                flops=10**9,
            )(*partial_rows, beams, *[held[slot] for slot in range(SET - 2)], *far, *near),
        )
    partial_rows = partial_rows[0]

    pieces = lax.all_to_all(partial_rows, "pulse", 0, 0, tiled=True)
    doubled = call(
        sum_kernel, jax.ShapeDtypeStruct((sets, 2, piece, 2 * width), half_type), [VMEM]
    )(pieces)

    def device(pulse, u, i):
        return pulse * tiles + u * SET + swapped(i)

    crossing = []
    for a in range(groups):
        for b in range(a + 1, groups):
            crossing.append([device(*end) for u in range(sets) for end in ((a, u, b), (b, u, a))])
    for a in range(0, groups, 2):
        crossing.append(
            [device(*end) for u in range(sets) for end in ((a, u, a), (a + 1, u, a + 1))]
        )
    last = lax.all_to_all(
        doubled.reshape(2 * sets, piece, 2 * width),
        ("pulse", "tile"),
        0,
        0,
        axis_index_groups=crossing,
        tiled=True,
    )
    return call(
        last_kernel, jax.ShapeDtypeStruct((piece, 2 * width), jnp.float32), [SMEM, VMEM]
    )(where, last)


def solution(mesh):
    placed = (
        P(None, None, ("pulse", "tile")),
        P(),
        P(),
        P(),
        P(),
        P("pulse", "tile", None, None, None),
    )
    return jax.shard_map(
        body, mesh=mesh, in_specs=placed, out_specs=P(("pulse", "tile"), None), check_vma=False
    )
```
